128 devices in a mesh: data: 1, cp: 64 (over z, y, x), tp: 2 (over core).
Axes of the slice: x: 4, y: 4, z: 4, core: 2. Of those that a mesh axis runs over, the one named last changes fastest.
Arguments:
- x_in: bfloat16 [16384, 2048], P(('data', 'cp', 'tp'))
- w_q: bfloat16 [2048, 32, 128], P(None, 'tp')
- w_k: bfloat16 [2048, 4, 128], P(None, 'tp')
- w_v: bfloat16 [2048, 4, 128], P(None, 'tp')
- w_o: bfloat16 [32, 128, 2048], P('tp')
- expert_idx: int32 [16384, 2], P(('data', 'cp', 'tp'))
- gate_wts: float32 [16384, 2], P(('data', 'cp', 'tp'))
- w_gate: bfloat16 [128, 2048, 768], P(('cp', 'tp'))
- w_up: bfloat16 [128, 2048, 768], P(('cp', 'tp'))
- w_down: bfloat16 [128, 768, 2048], P(('cp', 'tp'))
Outputs:
- output: bfloat16 [16384, 2048], P(('data', 'cp', 'tp'))
All inputs are finite; a program needn't handle non-finite values.
Results may differ from the reference program's by a relative error of at most 0.0101173.
Values are sent between devices in bfloat16 or wider.
A program may use at most 1 GiB of HBM per device.

```python
import math
import jax
import jax.numpy as jnp
import numpy as np
from jax import lax

D = 2048
FF = 768
HEADS = 32
KV_HEADS = 4
HEAD = 128
EXPERTS = 128
TOK_DEV = 128
CP_SIZE = 64
TP_SIZE = 2

NUM_DEVS = CP_SIZE * TP_SIZE
SEQ_LEN = TOK_DEV * NUM_DEVS
HALF_ROWS = TOK_DEV // 2
SEG_LEN = HALF_ROWS * TP_SIZE
CAPACITY = 4 * TOK_DEV // EXPERTS
Q_PER_KV = HEADS // KV_HEADS


def draw_routing(key):
    key_hot, key_src = jax.random.split(key)
    rest_cnt = 2 * TOK_DEV - 2 * CAPACITY
    base_cnt, extra_cnt = divmod(rest_cnt, EXPERTS - 2)
    counts = [CAPACITY, CAPACITY] + [base_cnt + 1] * extra_cnt + [base_cnt] * (EXPERTS - 2 - extra_cnt)
    rank_table = np.repeat(np.arange(EXPERTS), counts)
    rank_ids = jnp.asarray(rank_table).astype(jnp.int32)
    hot_pair = jnp.asarray(rank_table[:TOK_DEV] < 2).astype(jnp.int32)
    expert_perm = jax.random.permutation(key_hot, EXPERTS)

    def one_source(src_dev):
        key_perm, key_rank, key_swap = jax.random.split(jax.random.fold_in(key_src, src_dev), 3)
        cold_ids = expert_perm[2:][jax.random.permutation(key_perm, EXPERTS - 2)]
        id_table = jnp.concatenate([expert_perm[:2], cold_ids])
        choice_ids = id_table[rank_ids]
        rand_rank = jax.random.permutation(key_rank, TOK_DEV)
        pair_score = (rand_rank + hot_pair * (TOK_DEV // 2)) * TOK_DEV + rand_rank
        pair_order = jnp.argsort(pair_score)
        first_ids = choice_ids[:TOK_DEV][pair_order]
        second = choice_ids[TOK_DEV:][pair_order]
        swap_flag = jax.random.randint(key_swap, (TOK_DEV,), 0, 2) == 1
        return jnp.stack([jnp.where(swap_flag, second, first_ids), jnp.where(swap_flag, first_ids, second)], axis=1)

    return jax.vmap(one_source)(jnp.arange(NUM_DEVS)).reshape(SEQ_LEN, 2).astype(jnp.int32)


def row_positions():
    rows_all = jnp.arange(SEQ_LEN)
    dev_index = rows_all // TOK_DEV
    cp_rank = dev_index // TP_SIZE
    tp_rank = dev_index % TP_SIZE
    within = rows_all % TOK_DEV
    seg_index = jnp.where(within < HALF_ROWS, cp_rank, 2 * CP_SIZE - 1 - cp_rank)
    return seg_index * SEG_LEN + tp_rank * HALF_ROWS + within % HALF_ROWS


def setup_inputs(seed: int = 0, part: int = 0) -> dict:
    key_q, key_k, key_v, key_o, key_g, key_u, key_d = jax.random.split(jax.random.key(seed), 7)
    key_x, key_route, key_gate = jax.random.split(jax.random.fold_in(jax.random.key(seed + 1), part), 3)
    score_gain = math.sqrt(0.8 * math.log(SEQ_LEN))
    x_in = jax.random.normal(key_x, (SEQ_LEN, D), jnp.float32)
    w_q = jax.random.normal(key_q, (D, HEADS, HEAD), jnp.float32) * (score_gain / math.sqrt(D))
    w_k = jax.random.normal(key_k, (D, KV_HEADS, HEAD), jnp.float32) / math.sqrt(D)
    w_v = jax.random.normal(key_v, (D, KV_HEADS, HEAD), jnp.float32) / math.sqrt(D)
    w_o = jax.random.normal(key_o, (HEADS, HEAD, D), jnp.float32) / math.sqrt(HEADS * HEAD)
    w_gate = jax.random.normal(key_g, (EXPERTS, D, FF), jnp.float32) / math.sqrt(D)
    w_up = jax.random.normal(key_u, (EXPERTS, D, FF), jnp.float32) / math.sqrt(D)
    w_down = jax.random.normal(key_d, (EXPERTS, FF, D), jnp.float32) * (1.5 / math.sqrt(FF))
    gate_wts = jax.random.uniform(key_gate, (SEQ_LEN, 2), jnp.float32, 0.3, 0.7)
    return {'x_in': x_in.astype(jnp.bfloat16), 'w_q': w_q.astype(jnp.bfloat16), 'w_k': w_k.astype(jnp.bfloat16), 'w_v': w_v.astype(jnp.bfloat16), 'w_o': w_o.astype(jnp.bfloat16), 'expert_idx': draw_routing(key_route), 'gate_wts': gate_wts, 'w_gate': w_gate.astype(jnp.bfloat16), 'w_up': w_up.astype(jnp.bfloat16), 'w_down': w_down.astype(jnp.bfloat16)}


def reference(x_in, w_q, w_k, w_v, w_o, expert_idx, gate_wts, w_gate, w_up, w_down):
    positions = row_positions()
    queries = jnp.dot(x_in, w_q.reshape(D, HEADS * HEAD), preferred_element_type=jnp.float32).astype(jnp.bfloat16)
    keys_all = jnp.dot(x_in, w_k.reshape(D, KV_HEADS * HEAD), preferred_element_type=jnp.float32).astype(jnp.bfloat16)
    keys_all = keys_all.reshape(SEQ_LEN, KV_HEADS, HEAD).astype(jnp.float32)
    values_all = jnp.dot(x_in, w_v.reshape(D, KV_HEADS * HEAD), preferred_element_type=jnp.float32).astype(jnp.bfloat16)
    values_all = values_all.reshape(SEQ_LEN, KV_HEADS, HEAD).astype(jnp.float32)
    att_scale = 1.0 / math.sqrt(HEAD)

    def attend(q_inputs):
        q_block, q_pos = q_inputs
        scores = jnp.einsum('qngc,knc->ngqk', q_block.astype(jnp.float32), keys_all) * att_scale
        scores = jnp.where(positions[None, None, None, :] <= q_pos[None, None, :, None], scores, -jnp.inf)
        exp_scores = jnp.exp(scores - jnp.max(scores, axis=-1, keepdims=True))
        attn_prob = (exp_scores / jnp.sum(exp_scores, axis=-1, keepdims=True)).astype(jnp.bfloat16)
        head_out = jnp.einsum('ngqk,knc->qngc', attn_prob.astype(jnp.float32), values_all)
        return head_out.astype(jnp.bfloat16).reshape(TOK_DEV, HEADS * HEAD)

    head_rows = lax.map(attend, (queries.reshape(NUM_DEVS, TOK_DEV, KV_HEADS, Q_PER_KV, HEAD), positions.reshape(NUM_DEVS, TOK_DEV)))
    attn_out = jnp.dot(head_rows.reshape(SEQ_LEN, HEADS * HEAD), w_o.reshape(HEADS * HEAD, D), preferred_element_type=jnp.float32)
    hidden = (x_in.astype(jnp.float32) + attn_out).astype(jnp.bfloat16)

    flat_ids = expert_idx.reshape(NUM_DEVS, 2 * TOK_DEV)
    onehot = (flat_ids[:, :, None] == jnp.arange(EXPERTS)[None, None, :]).astype(jnp.int32)
    slot_pos = jnp.sum(jnp.cumsum(onehot, axis=1) * onehot, axis=2) - 1
    source = jnp.arange(NUM_DEVS)[:, None]
    dest_row = ((flat_ids * NUM_DEVS + source) * CAPACITY + slot_pos).reshape(-1)
    buffer = jnp.zeros((EXPERTS * NUM_DEVS * CAPACITY, D), jnp.bfloat16).at[dest_row].set(jnp.repeat(hidden, 2, axis=0))

    def expert_ffn(expert_in):
        tok_rows, gate_w, up_w, down_w = expert_in
        gate_pre = jnp.dot(tok_rows, gate_w, preferred_element_type=jnp.float32)
        up_pre = jnp.dot(tok_rows, up_w, preferred_element_type=jnp.float32)
        hid_act = (jax.nn.silu(gate_pre) * up_pre).astype(jnp.bfloat16)
        return jnp.dot(hid_act, down_w, preferred_element_type=jnp.float32).astype(jnp.bfloat16)

    expert_out = lax.map(expert_ffn, (buffer.reshape(EXPERTS, NUM_DEVS * CAPACITY, D), w_gate, w_up, w_down))
    picked = expert_out.reshape(-1, D)[dest_row].reshape(SEQ_LEN, 2, D).astype(jnp.float32)
    moe_out = jnp.sum(gate_wts[:, :, None] * picked, axis=1)
    return (hidden.astype(jnp.float32) + moe_out).astype(jnp.bfloat16)
```

```python
import functools
import math

import jax
import jax.numpy as jnp
from jax import lax
from jax.experimental import pallas as pl
from jax.experimental.pallas import tpu as pltpu
from jax.sharding import PartitionSpec as P

NEG = -1e30


def flash_kernel(heads, scale2, q_ref, kv_hbm, o_ref, kv_v, acc_s, m_s, l_s, sems):
    r = lax.axis_index('cp')
    n_seg = kv_hbm.shape[0]
    seg = kv_hbm.shape[2]
    half = seg // 2
    per = 8
    n_chunk = n_seg // per
    keys = per * seg

    def chunk_copy(h, c):
        return pltpu.make_async_copy(kv_hbm.at[pl.ds(c * per, per), h], kv_v.at[h, pl.ds(c * per, per)], sems.at[h, c])

    for h in range(2):
        for c in range(n_chunk):
            chunk_copy(h, c).start()

    acc_s[...] = jnp.zeros_like(acc_s)
    l_s[...] = jnp.zeros_like(l_s)
    m_s[...] = jnp.full_like(m_s, NEG)
    n_pair = heads // 2
    rows = 2 * seg

    def q_tile(qs, hc):
        parts = []
        for j in range(2):
            col = (2 * hc + j) * 128
            for t in range(2):
                lo = t * seg + qs * half
                parts.append(q_ref[lo:lo + half, col:col + 128])
        return jnp.concatenate(parts, axis=0)

    def process(qs, h, c, masked):
        blk = kv_v.at[h, pl.ds(c * per, per)]
        kt = jnp.concatenate([blk[j, :, 0:128] for j in range(per)], axis=1)
        val = jnp.concatenate([blk[j, :, 128:256] for j in range(per)], axis=0)
        if masked:
            col = lax.broadcasted_iota(jnp.int32, (rows, keys), 1)
            row = lax.broadcasted_iota(jnp.int32, (rows, keys), 0) % seg
            kseg = c * per + col // seg
            if h == 0:
                ok = (kseg < r) | ((kseg == r) & (col % seg <= row))
            else:
                ok = (kseg > r) | ((kseg == r) & (col % seg <= row))
        for hc in range(n_pair):
            at = pl.ds((qs * n_pair + hc) * rows, rows)
            s = jnp.dot(q_tile(qs, hc), kt, preferred_element_type=jnp.float32)
            if masked:
                s = jnp.where(ok, s, NEG)
            m_prev = m_s[at, :]
            m_new = jnp.maximum(m_prev, jnp.max(s, axis=1, keepdims=True) * scale2)
            alpha = jnp.exp2(m_prev - m_new)
            p = jnp.exp2(s * scale2 - m_new[:, 0:1])
            m_s[at, :] = m_new
            lp = p[:, 0:128]
            for j in range(1, keys // 128):
                lp = lp + p[:, j * 128:(j + 1) * 128]
            l_s[at, :] = l_s[at, :] * alpha + lp
            acc_s[at, :] = acc_s[at, :] * alpha + jnp.dot(p.astype(jnp.bfloat16), val, preferred_element_type=jnp.float32)

    edge = r // per

    def low_body(c, _):
        process(1, 0, c, False)
        return 0

    for c in range(n_chunk):
        chunk_copy(0, c).wait()
    lax.fori_loop(0, n_chunk, low_body, 0)

    def low2_body(c, _):
        process(0, 0, c, False)
        return 0

    lax.fori_loop(0, edge, low2_body, 0)
    process(0, 0, edge, True)
    for c in range(n_chunk):
        chunk_copy(1, c).wait()
    process(1, 1, edge, True)

    def high_body(c, _):
        process(1, 1, c, False)
        return 0

    lax.fori_loop(edge + 1, n_chunk, high_body, 0)

    for qs in range(2):
        for hc in range(n_pair):
            at = pl.ds((qs * n_pair + hc) * rows, rows)
            out = (acc_s[at, :] / jnp.sum(l_s[at, :], axis=1, keepdims=True)).astype(o_ref.dtype)
            for j in range(2):
                col = (2 * hc + j) * 128
                for t in range(2):
                    lo = t * seg + qs * half
                    o_ref[lo:lo + half, col:col + 128] = out[(j * 2 + t) * half:(j * 2 + t + 1) * half]


def flash(q, kv, heads, n_idx):
    rows = q.shape[0]
    n_seg, _, seg, _ = kv.shape
    m_rows = heads * rows
    scale2 = (128 ** -0.5) * math.log2(math.e)
    pairs = heads * (n_seg * 2 + 1) * seg * seg
    return pl.pallas_call(
        functools.partial(flash_kernel, heads, scale2),
        out_shape=jax.ShapeDtypeStruct((rows, heads * 128), jnp.bfloat16),
        grid=(1,),
        in_specs=[pl.BlockSpec((rows, heads * 128), lambda i: (0, n_idx)), pl.BlockSpec(memory_space=pl.ANY)],
        out_specs=pl.BlockSpec((rows, heads * 128), lambda i: (0, 0)),
        scratch_shapes=[
            pltpu.VMEM((2, n_seg, seg, 256), jnp.bfloat16),
            pltpu.VMEM((m_rows, 128), jnp.float32),
            pltpu.VMEM((m_rows, 128), jnp.float32),
            pltpu.VMEM((m_rows, 128), jnp.float32),
            pltpu.SemaphoreType.DMA((2, n_seg // 8)),
        ],
        compiler_params=pltpu.CompilerParams(vmem_limit_bytes=40 * 1024 * 1024),
        cost_estimate=pl.CostEstimate(flops=pairs * 128 * 4 * 2, bytes_accessed=n_seg * 2 * seg * 512, transcendentals=pairs),
        name='flash_head',
    )(q, kv)


def solution(mesh):
    cp_size = mesh.shape['cp']
    tp_size = mesh.shape['tp']
    num_devs = cp_size * tp_size
    row_spec = P(('data', 'cp', 'tp'), None)
    head_spec = P(None, 'tp', None)
    wo_spec = P('tp', None, None)
    expert_spec = P(('cp', 'tp'), None, None)

    def device_fn(x_blk, w_q, w_k, w_v, w_o, idx_blk, gate_blk, w_gate, w_up, w_down):
        tok_dev, d_model = x_blk.shape
        half = tok_dev // 2
        kv_local, head_dim = w_k.shape[1], w_k.shape[2]
        q_per_kv = w_q.shape[1] // kv_local
        exp_local = w_gate.shape[0]
        num_exp = exp_local * num_devs
        capacity = 4 * tok_dev // num_exp

        x_rows = lax.all_gather(x_blk, 'tp', axis=0, tiled=True)
        x_seg = x_rows.reshape(2, 2, half, d_model).swapaxes(0, 1).reshape(2 * tok_dev, d_model)
        kv_heads = []
        for n in range(kv_local):
            key_t = jnp.einsum('mc,sm->cs', w_k[:, n], x_seg, preferred_element_type=jnp.float32).astype(jnp.bfloat16)
            val = jnp.einsum('sm,mc->sc', x_seg, w_v[:, n], preferred_element_type=jnp.float32).astype(jnp.bfloat16)
            segs = [jnp.concatenate([key_t[:, h * tok_dev:(h + 1) * tok_dev], val[h * tok_dev:(h + 1) * tok_dev]], axis=1) for h in range(2)]
            kv_heads.append(lax.all_gather(jnp.stack(segs), 'cp', axis=0, tiled=False))
        queries = jnp.dot(x_rows, w_q.reshape(d_model, -1), preferred_element_type=jnp.float32).astype(jnp.bfloat16)
        head_out = [flash(queries, kv_heads[n], q_per_kv, n) for n in range(kv_local)]
        head_out = jnp.concatenate(head_out, axis=1)
        part_sum = jnp.dot(head_out, w_o.reshape(-1, d_model), preferred_element_type=jnp.float32)
        attn_out = lax.psum_scatter(part_sum, 'tp', scatter_dimension=0, tiled=True)
        hidden = (x_blk.astype(jnp.float32) + attn_out).astype(jnp.bfloat16)

        flat_ids = idx_blk.reshape(-1)
        onehot = (flat_ids[:, None] == jnp.arange(num_exp)[None, :]).astype(jnp.int32)
        slot_pos = jnp.sum(jnp.cumsum(onehot, axis=0) * onehot, axis=1) - 1
        slot_ids = (flat_ids * capacity + slot_pos).reshape(tok_dev, 2)
        select = (slot_ids[:, :, None] == jnp.arange(num_exp * capacity)[None, None, :]).astype(jnp.bfloat16)
        send_buf = jnp.einsum('tkn,tm->nm', select, hidden, preferred_element_type=jnp.float32).astype(jnp.bfloat16)
        recv_buf = lax.all_to_all(send_buf, ('cp', 'tp'), 0, 0, tiled=True)
        tok_in = recv_buf.reshape(num_devs, exp_local, capacity, -1)
        gate_pre = jnp.einsum('secm,emf->secf', tok_in, w_gate, preferred_element_type=jnp.float32)
        up_pre = jnp.einsum('secm,emf->secf', tok_in, w_up, preferred_element_type=jnp.float32)
        hid_act = (jax.nn.silu(gate_pre) * up_pre).astype(jnp.bfloat16)
        exp_out = jnp.einsum('secf,efm->secm', hid_act, w_down, preferred_element_type=jnp.float32).astype(jnp.bfloat16)
        back_buf = lax.all_to_all(exp_out.reshape(num_devs * exp_local * capacity, -1), ('cp', 'tp'), 0, 0, tiled=True)
        picked = jnp.einsum('tkn,nm->tkm', select, back_buf, preferred_element_type=jnp.float32)
        moe_out = jnp.sum(gate_blk[:, :, None] * picked, axis=1)
        return (hidden.astype(jnp.float32) + moe_out).astype(jnp.bfloat16)

    return jax.shard_map(device_fn, mesh=mesh, in_specs=(row_spec, head_spec, head_spec, head_spec, wo_spec, row_spec, row_spec, expert_spec, expert_spec, expert_spec), out_specs=row_spec, check_vma=False)
```

```python
import functools
import math

import jax
import jax.numpy as jnp
from jax import lax
from jax.experimental import pallas as pl
from jax.experimental.pallas import tpu as pltpu
from jax.sharding import PartitionSpec as P

NEG = -1e30
MESH = pl.DeviceIdType.MESH
STEPS = (1, 3, 2)


def swap_kernel(x_ref, o_ref, buf, ssem, rsem):
    cp, tp = lax.axis_index('cp'), lax.axis_index('tp')
    peer = (0, cp, 1 - tp)
    rows = x_ref.shape[0]
    barrier = pltpu.get_barrier_semaphore()
    pl.semaphore_signal(barrier, inc=1, device_id=peer, device_id_type=MESH)
    pl.semaphore_wait(barrier, 1)
    copy = pltpu.make_async_remote_copy(src_ref=x_ref, dst_ref=buf, send_sem=ssem, recv_sem=rsem, device_id=peer, device_id_type=MESH)
    copy.start()
    o_ref[pl.ds(pl.multiple_of(tp * rows, rows), rows), :] = x_ref[...]
    copy.wait()
    o_ref[pl.ds(pl.multiple_of((1 - tp) * rows, rows), rows), :] = buf[...]


def swap_rows(x):
    rows, cols = x.shape
    return pl.pallas_call(
        swap_kernel,
        out_shape=jax.ShapeDtypeStruct((2 * rows, cols), x.dtype),
        in_specs=[pl.BlockSpec(memory_space=pltpu.VMEM)],
        out_specs=pl.BlockSpec(memory_space=pltpu.VMEM),
        scratch_shapes=[pltpu.VMEM((rows, cols), x.dtype), pltpu.SemaphoreType.DMA, pltpu.SemaphoreType.DMA],
        compiler_params=pltpu.CompilerParams(collective_id=1, has_side_effects=True),
        name='swap_rows',
    )(x)


def join_kernel(p_ref, x_ref, o_ref, buf, ssem, rsem):
    cp, tp = lax.axis_index('cp'), lax.axis_index('tp')
    peer = (0, cp, 1 - tp)
    rows = x_ref.shape[0]
    barrier = pltpu.get_barrier_semaphore()
    pl.semaphore_signal(barrier, inc=1, device_id=peer, device_id_type=MESH)
    pl.semaphore_wait(barrier, 1)
    away = p_ref.at[pl.ds(pl.multiple_of((1 - tp) * rows, rows), rows)]
    copy = pltpu.make_async_remote_copy(src_ref=away, dst_ref=buf, send_sem=ssem, recv_sem=rsem, device_id=peer, device_id_type=MESH)
    copy.start()
    copy.wait()
    mine = p_ref[pl.ds(pl.multiple_of(tp * rows, rows), rows), :]
    o_ref[...] = (x_ref[...].astype(jnp.float32) + (mine + buf[...])).astype(o_ref.dtype)


def join_parts(part, x):
    return pl.pallas_call(
        join_kernel,
        out_shape=jax.ShapeDtypeStruct(x.shape, x.dtype),
        in_specs=[pl.BlockSpec(memory_space=pltpu.VMEM)] * 2,
        out_specs=pl.BlockSpec(memory_space=pltpu.VMEM),
        scratch_shapes=[pltpu.VMEM(x.shape, jnp.float32), pltpu.SemaphoreType.DMA, pltpu.SemaphoreType.DMA],
        compiler_params=pltpu.CompilerParams(collective_id=2, has_side_effects=True),
        name='join_parts',
    )(part, x)


def ring_step(i):
    return 1 + 2 * i - 3 * (i // 2)


def attn_kernel(scale2, q_ref, kt_ref, v_ref, o_ref, qb, kb, vb, so, ob, acc_s, m_s, l_s,
                q_ss, k_ss, v_ss, o_ss, q_rs, kx_rs, vx_rs, o_rs, k_rs, v_rs, kp_rs, vp_rs, kd_ss, vd_ss, kf_ss, vf_ss, kp_ss, vp_ss):
    cp, c = lax.axis_index('cp'), lax.axis_index('tp')
    x, y, z = cp % 4, (cp // 4) % 4, cp // 16
    g = z * 4 + y
    seg = kt_ref.shape[-1]
    half = seg // 2
    wide = so.shape[-1]
    heads = wide // 128

    def dev(xx, yy, zz, t):
        return (0, (zz % 4) * 16 + (yy % 4) * 4 + xx % 4, t)

    barrier = pltpu.get_barrier_semaphore()
    for d in STEPS:
        for t in range(2):
            pl.semaphore_signal(barrier, inc=1, device_id=dev(x + d, y, z, t), device_id_type=MESH)
        pl.semaphore_signal(barrier, inc=1, device_id=dev(x, y + d, z, c), device_id_type=MESH)
        pl.semaphore_signal(barrier, inc=1, device_id=dev(x, y, z + d, c), device_id_type=MESH)
    pl.semaphore_signal(barrier, inc=1, device_id=dev(x, y, z, 1 - c), device_id_type=MESH)
    pl.semaphore_wait(barrier, 13)

    def move(src, dst, ssem, rsem, xx, t, start):
        here = (xx == x) & (t == c)
        far = pltpu.make_async_remote_copy(src_ref=src, dst_ref=dst, send_sem=ssem, recv_sem=rsem, device_id=dev(xx, y, z, t), device_id_type=MESH)

        @pl.when(jnp.logical_not(here))
        def _():
            if start:
                far.start()
            else:
                far.wait_send()

        if start:
            @pl.when(here)
            def _():
                pltpu.make_async_copy(src, dst, rsem).start()

    def exchange(start):
        for j in range(2):
            for t in range(2):
                i = j * 2 + t
                move(kt_ref.at[j, t], kb.at[t, g, x], k_ss.at[i], kx_rs, 2 * c + j, t, start)
                move(v_ref.at[j, t], vb.at[t, g, x], v_ss.at[i], vx_rs, 2 * c + j, t, start)
        for j in range(2):
            for t in range(2):
                i = j * 2 + t
                move(q_ref.at[:, pl.ds(i * wide, wide)], qb.at[x], q_ss.at[i], q_rs, 2 * c + j, t, start)

    def arrived(ref, sem):
        pltpu.make_async_copy(ref, ref, sem).wait()

    def push(buf, gg, yy, zz, t, ssem, rsem):
        pltpu.make_async_remote_copy(src_ref=buf.at[c, gg], dst_ref=buf.at[c, gg], send_sem=ssem, recv_sem=rsem.at[gg], device_id=dev(x, yy, zz, t), device_id_type=MESH).start()

    def to_partner(gg):
        push(kb, gg, y, z, 1 - c, kp_ss, kp_rs)
        push(vb, gg, y, z, 1 - c, vp_ss, vp_rs)

    exchange(True)
    arrived(kb.at[c, g], kx_rs)
    arrived(vb.at[c, g], vx_rs)
    for d in STEPS:
        push(kb, g, y + d, z, c, kd_ss, k_rs)
        push(vb, g, y + d, z, c, vd_ss, v_rs)
        push(kb, g, y, z + d, c, kd_ss, k_rs)
        push(vb, g, y, z + d, c, vd_ss, v_rs)
        if d == 1:
            to_partner(g)
    arrived(qb, q_rs)

    units = [(hh, xp) for hh in range(heads) for xp in range(2)]
    keys = 4 * seg
    rows = 2 * seg

    def q_unit(qs, hh, xp):
        parts = [qb[xx, pl.ds(pl.multiple_of(t * seg + qs * half, half), half), hh * 128:(hh + 1) * 128] for xx in (2 * xp, 2 * xp + 1) for t in range(2)]
        return jnp.concatenate(parts, axis=0)

    def tiles(gg, work):
        todo = []
        for qs, h, masked, first in work:
            kt = jnp.concatenate([kb[h, gg, i] for i in range(4)], axis=1)
            todo += [(qs, h, masked, first, kt, hh, xp) for hh, xp in units]

        def score(item):
            qs, h, masked, first, kt, hh, xp = item
            return jnp.dot(q_unit(qs, hh, xp), kt, preferred_element_type=jnp.float32)

        s_next = score(todo[0])
        for n, (qs, h, masked, first, kt, hh, xp) in enumerate(todo):
            s = s_next
            if n + 1 < len(todo):
                s_next = score(todo[n + 1])
            if masked:
                col = lax.broadcasted_iota(jnp.int32, (rows, keys), 1)
                row = lax.broadcasted_iota(jnp.int32, (rows, keys), 0) + xp * rows
                ck, cq = col // seg, row // seg
                before = (ck < cq) if h == 0 else (ck > cq)
                s = jnp.where(before | ((ck == cq) & (col % seg <= row % seg)), s, NEG)
            at = pl.ds(xp * rows, rows)
            m_new = jnp.broadcast_to(jnp.max(s, axis=1, keepdims=True) * scale2, (rows, 128))
            if not first:
                m_prev = m_s[qs, hh, at]
                m_new = jnp.maximum(m_prev, m_new)
                alpha = jnp.exp2(m_prev - m_new)
            m_s[qs, hh, at] = m_new
            ps = [jnp.exp2(s[:, i * 128:(i + 1) * 128] * scale2 - m_new) for i in range(4)]
            lp = (ps[0] + ps[1]) + (ps[2] + ps[3])
            p = jnp.concatenate([v.astype(jnp.bfloat16) for v in ps], axis=1)
            val = vb[h, gg].reshape(keys, 128)
            pv = jnp.dot(p, val, preferred_element_type=jnp.float32)
            if first:
                l_s[qs, hh, at] = lp
                acc_s[qs, hh, at] = pv
            else:
                l_s[qs, hh, at] = l_s[qs, hh, at] * alpha + lp
                acc_s[qs, hh, at] = acc_s[qs, hh, at] * alpha + pv

    def ready(gg):
        arrived(kb.at[1 - c, gg], kp_rs.at[gg])
        arrived(vb.at[1 - c, gg], vp_rs.at[gg])

    def later(gg):
        ready(gg)
        h = (gg > g).astype(jnp.int32)
        tiles(gg, [(1, 0, False, False), (h, h, False, False)])

    ready(g)
    tiles(g, [(1, 0, False, True), (0, 0, True, True), (1, 1, True, False)])

    def group(dy, dz):
        return ((z + 4 - dz) % 4) * 4 + (y + 4 - dy) % 4

    def pass_direct(i):
        d = ring_step(i)
        gy, gz = group(d, 0), group(0, d)
        for gg in (gy, gz):
            arrived(kb.at[c, gg], k_rs.at[gg])
            arrived(vb.at[c, gg], v_rs.at[gg])
            to_partner(gg)
        for e in STEPS:
            push(kb, gy, y, z + e, c, kf_ss, k_rs)
            push(vb, gz, y + e, z, c, vf_ss, v_rs)

    def direct(i, _):
        @pl.when(i < 2)
        def _():
            pass_direct(i + 1)
        d = ring_step(i)
        later(group(d, 0))
        later(group(0, d))
        return 0

    pass_direct(0)
    lax.fori_loop(0, 3, direct, 0)

    def corner(i):
        return group(ring_step(i // 3), ring_step(i % 3))

    def pass_corner(i):
        gg = corner(i)
        arrived(kb.at[c, gg], k_rs.at[gg])
        arrived(vb.at[c, gg], v_rs.at[gg])
        to_partner(gg)

    def corners(i, _):
        @pl.when(i < 8)
        def _():
            pass_corner(i + 1)
        later(corner(i))
        return 0

    pass_corner(0)
    lax.fori_loop(0, 9, corners, 0)

    for qs in range(2):
        for hh, xp in units:
            at = pl.ds(xp * rows, rows)
            out = (acc_s[qs, hh, at] / jnp.sum(l_s[qs, hh, at], axis=1, keepdims=True)).astype(so.dtype)
            for n, (xx, t) in enumerate([(xx, t) for xx in (2 * xp, 2 * xp + 1) for t in range(2)]):
                so[xx, t * seg + qs * half:t * seg + (qs + 1) * half, hh * 128:(hh + 1) * 128] = out[n * half:(n + 1) * half]

    def give_back(start):
        for i in range(4):
            cols = pl.ds(pl.multiple_of(((x % 2) * 2 + c) * wide, wide), wide)
            move(so.at[i], ob.at[:, cols], o_ss.at[i], o_rs, i, x // 2, start)

    give_back(True)
    arrived(ob, o_rs)
    o_ref[...] = ob[...]
    give_back(False)
    exchange(False)
    arrived(kb.at[0, pl.ds(0, 6)], kd_ss)
    arrived(vb.at[0, pl.ds(0, 6)], vd_ss)
    arrived(kb.at[0, pl.ds(0, 9)], kf_ss)
    arrived(vb.at[0, pl.ds(0, 9)], vf_ss)
    arrived(kb.at[0], kp_ss)
    arrived(vb.at[0], vp_ss)


def attention(q, kt, val):
    rows, cols = q.shape
    seg = kt.shape[-1]
    wide = cols // 4
    dma = pltpu.SemaphoreType.DMA
    bf, f32 = jnp.bfloat16, jnp.float32
    return pl.pallas_call(
        functools.partial(attn_kernel, (128 ** -0.5) * math.log2(math.e)),
        out_shape=jax.ShapeDtypeStruct((rows, cols), bf),
        in_specs=[pl.BlockSpec(memory_space=pltpu.VMEM)] * 3,
        out_specs=pl.BlockSpec(memory_space=pltpu.VMEM),
        scratch_shapes=[
            pltpu.VMEM((4, rows, wide), bf),
            pltpu.VMEM((2, 16, 4, seg, 128), bf),
            pltpu.VMEM((2, 16, 4, seg, 128), bf),
            pltpu.VMEM((4, rows, wide), bf),
            pltpu.VMEM((rows, cols), bf),
            pltpu.VMEM((2, wide // 128, 4 * seg, 128), f32),
            pltpu.VMEM((2, wide // 128, 4 * seg, 128), f32),
            pltpu.VMEM((2, wide // 128, 4 * seg, 128), f32),
            dma((4,)), dma((4,)), dma((4,)), dma((4,)),
            dma, dma, dma, dma,
            dma((16,)), dma((16,)), dma((16,)), dma((16,)),
            dma, dma, dma, dma, dma, dma,
        ],
        compiler_params=pltpu.CompilerParams(collective_id=3, has_side_effects=True, vmem_limit_bytes=48 * 1024 * 1024),
        name='ring_attention',
    )(q, kt, val)


def solution(mesh):
    cp_size = mesh.shape['cp']
    tp_size = mesh.shape['tp']
    num_devs = cp_size * tp_size
    row_spec = P(('data', 'cp', 'tp'), None)
    head_spec = P(None, 'tp', None)
    wo_spec = P('tp', None, None)
    expert_spec = P(('cp', 'tp'), None, None)

    def device_fn(x_blk, w_q, w_k, w_v, w_o, idx_blk, gate_blk, w_gate, w_up, w_down):
        tok_dev, d_model = x_blk.shape
        half = tok_dev // 2
        exp_local = w_gate.shape[0]
        num_exp = exp_local * num_devs
        capacity = 4 * tok_dev // num_exp

        x_rows = swap_rows(x_blk)
        x_seg = x_rows.reshape(2, 2, half, d_model).swapaxes(0, 1).reshape(2, tok_dev, d_model)
        key_t = jnp.einsum('mnc,hsm->nhcs', w_k, x_seg, preferred_element_type=jnp.float32).astype(jnp.bfloat16)
        val = jnp.einsum('hsm,mnc->nhsc', x_seg, w_v, preferred_element_type=jnp.float32).astype(jnp.bfloat16)
        queries = jnp.dot(x_rows, w_q.reshape(d_model, -1), preferred_element_type=jnp.float32).astype(jnp.bfloat16)
        head_out = attention(queries, key_t, val)
        part_sum = jnp.dot(head_out, w_o.reshape(-1, d_model), preferred_element_type=jnp.float32)
        hidden = join_parts(part_sum, x_blk)

        flat_ids = idx_blk.reshape(-1)
        onehot = (flat_ids[:, None] == jnp.arange(num_exp)[None, :]).astype(jnp.int32)
        slot_pos = jnp.sum(jnp.cumsum(onehot, axis=0) * onehot, axis=1) - 1
        slot_ids = (flat_ids * capacity + slot_pos).reshape(tok_dev, 2)
        select = (slot_ids[:, :, None] == jnp.arange(num_exp * capacity)[None, None, :]).astype(jnp.bfloat16)
        send_buf = jnp.einsum('tkn,tm->nm', select, hidden, preferred_element_type=jnp.float32).astype(jnp.bfloat16)
        recv_buf = lax.all_to_all(send_buf, ('cp', 'tp'), 0, 0, tiled=True)
        tok_in = recv_buf.reshape(num_devs, exp_local, capacity, -1)
        gate_pre = jnp.einsum('secm,emf->secf', tok_in, w_gate, preferred_element_type=jnp.float32)
        up_pre = jnp.einsum('secm,emf->secf', tok_in, w_up, preferred_element_type=jnp.float32)
        hid_act = (jax.nn.silu(gate_pre) * up_pre).astype(jnp.bfloat16)
        exp_out = jnp.einsum('secf,efm->secm', hid_act, w_down, preferred_element_type=jnp.float32).astype(jnp.bfloat16)
        back_buf = lax.all_to_all(exp_out.reshape(num_devs * exp_local * capacity, -1), ('cp', 'tp'), 0, 0, tiled=True)
        picked = jnp.einsum('tkn,nm->tkm', select, back_buf, preferred_element_type=jnp.float32)
        moe_out = jnp.sum(gate_blk[:, :, None] * picked, axis=1)
        return (hidden.astype(jnp.float32) + moe_out).astype(jnp.bfloat16)

    return jax.shard_map(device_fn, mesh=mesh, in_specs=(row_spec, head_spec, head_spec, head_spec, wo_spec, row_spec, row_spec, expert_spec, expert_spec, expert_spec), out_specs=row_spec, check_vma=False)
```

```python
import functools
import math

import jax
import jax.numpy as jnp
from jax import lax
from jax.experimental import pallas as pl
from jax.experimental.pallas import tpu as pltpu
from jax.sharding import PartitionSpec as P

NEG = -1e30
MESH = pl.DeviceIdType.MESH
STEPS = (1, 3, 2)


def swap_kernel(x_ref, o_ref, buf, ssem, rsem):
    cp, tp = lax.axis_index('cp'), lax.axis_index('tp')
    peer = (0, cp, 1 - tp)
    rows = x_ref.shape[0]
    barrier = pltpu.get_barrier_semaphore()
    pl.semaphore_signal(barrier, inc=1, device_id=peer, device_id_type=MESH)
    pl.semaphore_wait(barrier, 1)
    copy = pltpu.make_async_remote_copy(src_ref=x_ref, dst_ref=buf, send_sem=ssem, recv_sem=rsem, device_id=peer, device_id_type=MESH)
    copy.start()
    o_ref[pl.ds(pl.multiple_of(tp * rows, rows), rows), :] = x_ref[...]
    copy.wait()
    o_ref[pl.ds(pl.multiple_of((1 - tp) * rows, rows), rows), :] = buf[...]


def swap_rows(x):
    rows, cols = x.shape
    return pl.pallas_call(
        swap_kernel,
        out_shape=jax.ShapeDtypeStruct((2 * rows, cols), x.dtype),
        in_specs=[pl.BlockSpec(memory_space=pltpu.VMEM)],
        out_specs=pl.BlockSpec(memory_space=pltpu.VMEM),
        scratch_shapes=[pltpu.VMEM((rows, cols), x.dtype), pltpu.SemaphoreType.DMA, pltpu.SemaphoreType.DMA],
        compiler_params=pltpu.CompilerParams(collective_id=1, has_side_effects=True),
        name='swap_rows',
    )(x)


def join_kernel(p_ref, x_ref, o_ref, buf, ssem, rsem):
    cp, tp = lax.axis_index('cp'), lax.axis_index('tp')
    peer = (0, cp, 1 - tp)
    rows = x_ref.shape[0]
    barrier = pltpu.get_barrier_semaphore()
    pl.semaphore_signal(barrier, inc=1, device_id=peer, device_id_type=MESH)
    pl.semaphore_wait(barrier, 1)
    away = p_ref.at[pl.ds(pl.multiple_of((1 - tp) * rows, rows), rows)]
    copy = pltpu.make_async_remote_copy(src_ref=away, dst_ref=buf, send_sem=ssem, recv_sem=rsem, device_id=peer, device_id_type=MESH)
    copy.start()
    copy.wait()
    mine = p_ref[pl.ds(pl.multiple_of(tp * rows, rows), rows), :]
    o_ref[...] = (x_ref[...].astype(jnp.float32) + (mine + buf[...])).astype(o_ref.dtype)


def join_parts(part, x):
    return pl.pallas_call(
        join_kernel,
        out_shape=jax.ShapeDtypeStruct(x.shape, x.dtype),
        in_specs=[pl.BlockSpec(memory_space=pltpu.VMEM)] * 2,
        out_specs=pl.BlockSpec(memory_space=pltpu.VMEM),
        scratch_shapes=[pltpu.VMEM(x.shape, jnp.float32), pltpu.SemaphoreType.DMA, pltpu.SemaphoreType.DMA],
        compiler_params=pltpu.CompilerParams(collective_id=2, has_side_effects=True),
        name='join_parts',
    )(part, x)


def ring_step(i):
    return 1 + 2 * i - 3 * (i // 2)


def attn_kernel(scale2, q_ref, kt_ref, v_ref, o_ref, qb, kb, vb, so, ob, acc_s, m_s, l_s,
                q_ss, k_ss, v_ss, o_ss, q_rs, kx_rs, vx_rs, o_rs, k_rs, v_rs, kp_rs, vp_rs, kd_ss, vd_ss, kf_ss, vf_ss, kp_ss, vp_ss):
    cp, c = lax.axis_index('cp'), lax.axis_index('tp')
    x, y, z = cp % 4, (cp // 4) % 4, cp // 16
    g = z * 4 + y
    seg = kt_ref.shape[-1]
    half = seg // 2
    wide = so.shape[-1]
    heads = wide // 128

    def dev(xx, yy, zz, t):
        return (0, (zz % 4) * 16 + (yy % 4) * 4 + xx % 4, t)

    barrier = pltpu.get_barrier_semaphore()
    for d in STEPS:
        for t in range(2):
            pl.semaphore_signal(barrier, inc=1, device_id=dev(x + d, y, z, t), device_id_type=MESH)
        pl.semaphore_signal(barrier, inc=1, device_id=dev(x, y + d, z, c), device_id_type=MESH)
        pl.semaphore_signal(barrier, inc=1, device_id=dev(x, y, z + d, c), device_id_type=MESH)
    pl.semaphore_signal(barrier, inc=1, device_id=dev(x, y, z, 1 - c), device_id_type=MESH)
    pl.semaphore_wait(barrier, 13)

    def move(src, dst, ssem, rsem, xx, t, start):
        here = (xx == x) & (t == c)
        far = pltpu.make_async_remote_copy(src_ref=src, dst_ref=dst, send_sem=ssem, recv_sem=rsem, device_id=dev(xx, y, z, t), device_id_type=MESH)

        @pl.when(jnp.logical_not(here))
        def _():
            if start:
                far.start()
            else:
                far.wait_send()

        if start:
            @pl.when(here)
            def _():
                pltpu.make_async_copy(src, dst, rsem).start()

    def exchange(start):
        for j in range(2):
            for t in range(2):
                i = j * 2 + t
                move(kt_ref.at[j, t], kb.at[t, g, x], k_ss.at[i], kx_rs, 2 * c + j, t, start)
                move(v_ref.at[j, t], vb.at[t, g, x], v_ss.at[i], vx_rs, 2 * c + j, t, start)
        for j in range(2):
            for t in range(2):
                i = j * 2 + t
                move(q_ref.at[:, pl.ds(i * wide, wide)], qb.at[x], q_ss.at[i], q_rs, 2 * c + j, t, start)

    def arrived(ref, sem):
        pltpu.make_async_copy(ref, ref, sem).wait()

    def push(buf, gg, yy, zz, t, ssem, rsem):
        pltpu.make_async_remote_copy(src_ref=buf.at[c, gg], dst_ref=buf.at[c, gg], send_sem=ssem, recv_sem=rsem.at[gg], device_id=dev(x, yy, zz, t), device_id_type=MESH).start()

    def to_partner(gg):
        push(kb, gg, y, z, 1 - c, kp_ss, kp_rs)
        push(vb, gg, y, z, 1 - c, vp_ss, vp_rs)

    exchange(True)
    arrived(kb.at[c, g], kx_rs)
    arrived(vb.at[c, g], vx_rs)
    for d in STEPS:
        push(kb, g, y + d, z, c, kd_ss, k_rs)
        push(vb, g, y + d, z, c, vd_ss, v_rs)
        push(kb, g, y, z + d, c, kd_ss, k_rs)
        push(vb, g, y, z + d, c, vd_ss, v_rs)
        if d == 1:
            to_partner(g)
    arrived(qb, q_rs)

    units = [(hh, xp) for hh in range(heads) for xp in range(2)]
    keys = 4 * seg
    rows = 2 * seg

    def q_unit(qs, hh, xp):
        parts = [qb[xx, pl.ds(pl.multiple_of(t * seg + qs * half, half), half), hh * 128:(hh + 1) * 128] for xx in (2 * xp, 2 * xp + 1) for t in range(2)]
        return jnp.concatenate(parts, axis=0)

    def tiles(gg, work):
        todo = []
        for qs, h, masked, first in work:
            kt = jnp.concatenate([kb[h, gg, i] for i in range(4)], axis=1)
            todo += [(qs, h, masked, first, kt, hh, xp) for hh, xp in units]

        def score(item):
            qs, h, masked, first, kt, hh, xp = item
            return jnp.dot(q_unit(qs, hh, xp), kt, preferred_element_type=jnp.float32)

        s_next = score(todo[0])
        for n, (qs, h, masked, first, kt, hh, xp) in enumerate(todo):
            s = s_next
            if n + 1 < len(todo):
                s_next = score(todo[n + 1])
            if masked:
                col = lax.broadcasted_iota(jnp.int32, (rows, keys), 1)
                row = lax.broadcasted_iota(jnp.int32, (rows, keys), 0) + xp * rows
                ck, cq = col // seg, row // seg
                before = (ck < cq) if h == 0 else (ck > cq)
                s = jnp.where(before | ((ck == cq) & (col % seg <= row % seg)), s, NEG)
            at = pl.ds(xp * rows, rows)
            m_new = jnp.broadcast_to(jnp.max(s, axis=1, keepdims=True) * scale2, (rows, 128))
            if not first:
                m_prev = m_s[qs, hh, at]
                m_new = jnp.maximum(m_prev, m_new)
                alpha = jnp.exp2(m_prev - m_new)
            m_s[qs, hh, at] = m_new
            ps = [jnp.exp2(s[:, i * 128:(i + 1) * 128] * scale2 - m_new) for i in range(4)]
            lp = (ps[0] + ps[1]) + (ps[2] + ps[3])
            p = jnp.concatenate([v.astype(jnp.bfloat16) for v in ps], axis=1)
            val = vb[h, gg].reshape(keys, 128)
            pv = jnp.dot(p, val, preferred_element_type=jnp.float32)
            if first:
                l_s[qs, hh, at] = lp
                acc_s[qs, hh, at] = pv
            else:
                l_s[qs, hh, at] = l_s[qs, hh, at] * alpha + lp
                acc_s[qs, hh, at] = acc_s[qs, hh, at] * alpha + pv

    def ready(gg):
        arrived(kb.at[1 - c, gg], kp_rs.at[gg])
        arrived(vb.at[1 - c, gg], vp_rs.at[gg])

    def later(gg):
        ready(gg)
        h = (gg > g).astype(jnp.int32)
        tiles(gg, [(1, 0, False, False), (h, h, False, False)])

    ready(g)
    tiles(g, [(1, 0, False, True), (0, 0, True, True), (1, 1, True, False)])

    def group(dy, dz):
        return ((z + 4 - dz) % 4) * 4 + (y + 4 - dy) % 4

    def pass_direct(i):
        d = ring_step(i)
        gy, gz = group(d, 0), group(0, d)
        for gg in (gy, gz):
            arrived(kb.at[c, gg], k_rs.at[gg])
            arrived(vb.at[c, gg], v_rs.at[gg])
            to_partner(gg)
        for e in STEPS:
            push(kb, gy, y, z + e, c, kf_ss, k_rs)
            push(vb, gz, y + e, z, c, vf_ss, v_rs)

    def direct(i, _):
        @pl.when(i < 2)
        def _():
            pass_direct(i + 1)
        d = ring_step(i)
        later(group(d, 0))
        later(group(0, d))
        return 0

    pass_direct(0)
    lax.fori_loop(0, 3, direct, 0)

    def corner(i):
        return group(ring_step(i // 3), ring_step(i % 3))

    def pass_corner(i):
        gg = corner(i)
        arrived(kb.at[c, gg], k_rs.at[gg])
        arrived(vb.at[c, gg], v_rs.at[gg])
        to_partner(gg)

    def corners(i, _):
        @pl.when(i < 8)
        def _():
            pass_corner(i + 1)
        later(corner(i))
        return 0

    pass_corner(0)
    lax.fori_loop(0, 9, corners, 0)

    for qs in range(2):
        for hh, xp in units:
            at = pl.ds(xp * rows, rows)
            out = (acc_s[qs, hh, at] / jnp.sum(l_s[qs, hh, at], axis=1, keepdims=True)).astype(so.dtype)
            for n, (xx, t) in enumerate([(xx, t) for xx in (2 * xp, 2 * xp + 1) for t in range(2)]):
                so[xx, t * seg + qs * half:t * seg + (qs + 1) * half, hh * 128:(hh + 1) * 128] = out[n * half:(n + 1) * half]

    def give_back(start):
        for i in range(4):
            cols = pl.ds(pl.multiple_of(((x % 2) * 2 + c) * wide, wide), wide)
            move(so.at[i], ob.at[:, cols], o_ss.at[i], o_rs, i, x // 2, start)

    give_back(True)
    arrived(ob, o_rs)
    o_ref[...] = ob[...]
    give_back(False)
    exchange(False)
    arrived(kb.at[0, pl.ds(0, 6)], kd_ss)
    arrived(vb.at[0, pl.ds(0, 6)], vd_ss)
    arrived(kb.at[0, pl.ds(0, 9)], kf_ss)
    arrived(vb.at[0, pl.ds(0, 9)], vf_ss)
    arrived(kb.at[0], kp_ss)
    arrived(vb.at[0], vp_ss)


def attention(q, kt, val):
    rows, cols = q.shape
    seg = kt.shape[-1]
    wide = cols // 4
    dma = pltpu.SemaphoreType.DMA
    bf, f32 = jnp.bfloat16, jnp.float32
    return pl.pallas_call(
        functools.partial(attn_kernel, (128 ** -0.5) * math.log2(math.e)),
        out_shape=jax.ShapeDtypeStruct((rows, cols), bf),
        in_specs=[pl.BlockSpec(memory_space=pltpu.VMEM)] * 3,
        out_specs=pl.BlockSpec(memory_space=pltpu.VMEM),
        scratch_shapes=[
            pltpu.VMEM((4, rows, wide), bf),
            pltpu.VMEM((2, 16, 4, seg, 128), bf),
            pltpu.VMEM((2, 16, 4, seg, 128), bf),
            pltpu.VMEM((4, rows, wide), bf),
            pltpu.VMEM((rows, cols), bf),
            pltpu.VMEM((2, wide // 128, 4 * seg, 128), f32),
            pltpu.VMEM((2, wide // 128, 4 * seg, 128), f32),
            pltpu.VMEM((2, wide // 128, 4 * seg, 128), f32),
            dma((4,)), dma((4,)), dma((4,)), dma((4,)),
            dma, dma, dma, dma,
            dma((16,)), dma((16,)), dma((16,)), dma((16,)),
            dma, dma, dma, dma, dma, dma,
        ],
        compiler_params=pltpu.CompilerParams(collective_id=3, has_side_effects=True, vmem_limit_bytes=48 * 1024 * 1024),
        name='ring_attention',
    )(q, kt, val)


def moe_kernel(h_ref, st_ref, s_ref, g_ref, wg_hbm, wu_hbm, wd_hbm, y_ref, send, recv, res, back, wg, wu, wd, w_sem, hop, s_ss, s_rs, r_ss, r_rs):
    cp, tp = lax.axis_index('cp'), lax.axis_index('tp')
    me = cp * 2 + tp
    x, y, z = cp % 4, (cp // 4) % 4, cp // 16
    n_dev, cap, width = send.shape
    n_grp = s_rs.shape[0]
    per = n_dev // n_grp
    rows = per * cap

    def dev(xx, yy, zz, t):
        return (0, (zz % 4) * 16 + (yy % 4) * 4 + xx % 4, t)

    loads = [pltpu.make_async_copy(a, b, w_sem.at[i]) for i, (a, b) in enumerate(((wg_hbm, wg), (wu_hbm, wu), (wd_hbm, wd)))]
    for copy in loads:
        copy.start()
    barrier = pltpu.get_barrier_semaphore()
    for d in STEPS:
        pl.semaphore_signal(barrier, inc=1, device_id=dev(x + d, y, z, tp), device_id_type=MESH)
        pl.semaphore_signal(barrier, inc=1, device_id=dev(x, y + d, z, tp), device_id_type=MESH)
        pl.semaphore_signal(barrier, inc=1, device_id=dev(x, y, z + d, tp), device_id_type=MESH)
    pl.semaphore_signal(barrier, inc=1, device_id=dev(x, y, z, 1 - tp), device_id_type=MESH)

    def pack(lo):
        at = lax.broadcasted_iota(jnp.int32, (rows, st_ref.shape[1]), 0) + lo * rows
        pick = (at == st_ref[0:1, :]) | (at == st_ref[1:2, :])
        out = jnp.dot(pick.astype(jnp.bfloat16), h_ref[...], preferred_element_type=jnp.float32)
        send[pl.ds(lo * per, per)] = out.astype(jnp.bfloat16).reshape(per, cap, width)

    for lo in range(n_grp):
        pack(lo)

    pl.semaphore_wait(barrier, 10)
    for d in STEPS:
        pl.semaphore_signal(hop.at[0], inc=1, device_id=dev(x, y + d, z, tp), device_id_type=MESH)
    pl.semaphore_wait(hop.at[0], 3)
    for d in STEPS:
        pl.semaphore_signal(hop.at[1], inc=1, device_id=dev(x, y, z + d, tp), device_id_type=MESH)
    pl.semaphore_wait(hop.at[1], 3)
    pl.semaphore_signal(hop.at[2], inc=1, device_id=dev(x, y, z, 1 - tp), device_id_type=MESH)
    pl.semaphore_wait(hop.at[2], 1)

    def peer(k, sign):
        j = (k * 91) % n_dev
        xx = (x + sign * ((j // 2) % 4)) % 4
        yy = (y + sign * ((j // 8) % 4)) % 4
        zz = (z + sign * (j // 32)) % 4
        return zz * 16 + yy * 4 + xx, (tp + j) % 2

    def give(k, _):
        c, t = peer(k, 1)
        pltpu.make_async_remote_copy(src_ref=send.at[c * 2 + t], dst_ref=recv.at[k], send_sem=s_ss, recv_sem=s_rs.at[k // per], device_id=(0, c, t), device_id_type=MESH).start()
        return 0

    own = pltpu.make_async_copy(send.at[me], recv.at[0], s_rs.at[0])
    own.start()
    lax.fori_loop(1, n_dev, give, 0)
    for copy in loads:
        copy.wait()

    def answer(k, _):
        c, t = peer(k, 3)
        pltpu.make_async_remote_copy(src_ref=res.at[k], dst_ref=back.at[me], send_sem=r_ss, recv_sem=r_rs, device_id=(0, c, t), device_id_type=MESH).start()
        return 0

    def group(i, _):
        part = recv.at[pl.ds(i * per, per)]
        pltpu.make_async_copy(part, part, s_rs.at[i]).wait()
        rows_in = part[...].reshape(rows, width)
        gate = jnp.dot(rows_in, wg[...], preferred_element_type=jnp.float32)
        up = jnp.dot(rows_in, wu[...], preferred_element_type=jnp.float32)
        act = (jax.nn.silu(gate) * up).astype(jnp.bfloat16)
        out = jnp.dot(act, wd[...], preferred_element_type=jnp.float32)
        res[pl.ds(i * per, per)] = out.astype(jnp.bfloat16).reshape(per, cap, width)
        lax.fori_loop(jnp.maximum(i * per, 1), (i + 1) * per, answer, 0)
        return 0

    lax.fori_loop(0, n_grp, group, 0)
    own_back = pltpu.make_async_copy(res.at[0], back.at[me], r_rs)
    own_back.start()
    pltpu.make_async_copy(back, back, r_rs).wait()
    all_back = back[...].reshape(n_dev * cap, width)
    at = lax.broadcasted_iota(jnp.int32, (s_ref.shape[0], n_dev * cap), 1)
    total = h_ref[...].astype(jnp.float32)
    moe = None
    for j in range(2):
        pick = (at == s_ref[:, j:j + 1]).astype(jnp.bfloat16)
        term = g_ref[:, j:j + 1] * jnp.dot(pick, all_back, preferred_element_type=jnp.float32)
        moe = term if moe is None else moe + term
    y_ref[...] = (total + moe).astype(y_ref.dtype)
    most = send.at[pl.ds(1, n_dev - 1)]
    pltpu.make_async_copy(most, most, s_ss).wait()
    pltpu.make_async_copy(most, most, r_ss).wait()


def moe(hidden, slot_ids, gates, w_gate, w_up, w_down, cap):
    d_model, ff = w_gate.shape
    n_dev = 4 * hidden.shape[0] // cap
    dma = pltpu.SemaphoreType.DMA
    bf = jnp.bfloat16
    vm = pl.BlockSpec(memory_space=pltpu.VMEM)
    anyspace = pl.BlockSpec(memory_space=pl.ANY)
    buf = pltpu.VMEM((n_dev, cap, d_model), bf)
    n_grp = 4
    return pl.pallas_call(
        moe_kernel,
        out_shape=jax.ShapeDtypeStruct(hidden.shape, bf),
        in_specs=[vm] * 4 + [anyspace] * 3,
        out_specs=vm,
        scratch_shapes=[
            buf, buf, buf, buf,
            pltpu.VMEM((d_model, ff), bf), pltpu.VMEM((d_model, ff), bf), pltpu.VMEM((ff, d_model), bf),
            dma((3,)), pltpu.SemaphoreType.REGULAR((3,)), dma, dma((n_grp,)), dma, dma,
        ],
        compiler_params=pltpu.CompilerParams(collective_id=4, has_side_effects=True, vmem_limit_bytes=48 * 1024 * 1024),
        name='moe_exchange',
    )(hidden, slot_ids.T, slot_ids, gates, w_gate, w_up, w_down)


def solution(mesh):
    cp_size = mesh.shape['cp']
    tp_size = mesh.shape['tp']
    num_devs = cp_size * tp_size
    row_spec = P(('data', 'cp', 'tp'), None)
    head_spec = P(None, 'tp', None)
    wo_spec = P('tp', None, None)
    expert_spec = P(('cp', 'tp'), None, None)

    def device_fn(x_blk, w_q, w_k, w_v, w_o, idx_blk, gate_blk, w_gate, w_up, w_down):
        tok_dev, d_model = x_blk.shape
        half = tok_dev // 2
        exp_local = w_gate.shape[0]
        num_exp = exp_local * num_devs
        capacity = 4 * tok_dev // num_exp

        x_rows = swap_rows(x_blk)
        x_seg = x_rows.reshape(2, 2, half, d_model).swapaxes(0, 1).reshape(2, tok_dev, d_model)
        key_t = jnp.einsum('mnc,hsm->nhcs', w_k, x_seg, preferred_element_type=jnp.float32).astype(jnp.bfloat16)
        val = jnp.einsum('hsm,mnc->nhsc', x_seg, w_v, preferred_element_type=jnp.float32).astype(jnp.bfloat16)
        queries = jnp.dot(x_rows, w_q.reshape(d_model, -1), preferred_element_type=jnp.float32).astype(jnp.bfloat16)
        head_out = attention(queries, key_t, val)
        part_sum = jnp.dot(head_out, w_o.reshape(-1, d_model), preferred_element_type=jnp.float32)
        hidden = join_parts(part_sum, x_blk)

        flat_ids = idx_blk.reshape(-1)
        onehot = (flat_ids[:, None] == jnp.arange(num_exp)[None, :]).astype(jnp.int32)
        slot_pos = jnp.sum(jnp.cumsum(onehot, axis=0) * onehot, axis=1) - 1
        slot_ids = (flat_ids * capacity + slot_pos).reshape(tok_dev, 2)
        return moe(hidden, slot_ids, gate_blk, w_gate[0], w_up[0], w_down[0], capacity)

    return jax.shard_map(device_fn, mesh=mesh, in_specs=(row_spec, head_spec, head_spec, head_spec, wo_spec, row_spec, row_spec, expert_spec, expert_spec, expert_spec), out_specs=row_spec, check_vma=False)
```

```python
import functools
import math

import jax
import jax.numpy as jnp
from jax import lax
from jax.experimental import pallas as pl
from jax.experimental.pallas import tpu as pltpu
from jax.sharding import PartitionSpec as P

NEG = -1e30
MESH = pl.DeviceIdType.MESH
STEPS = (1, 3, 2)


def swap_kernel(x_ref, o_ref, buf, ssem, rsem):
    cp, tp = lax.axis_index('cp'), lax.axis_index('tp')
    peer = (0, cp, 1 - tp)
    rows = x_ref.shape[0]
    barrier = pltpu.get_barrier_semaphore()
    pl.semaphore_signal(barrier, inc=1, device_id=peer, device_id_type=MESH)
    pl.semaphore_wait(barrier, 1)
    copy = pltpu.make_async_remote_copy(src_ref=x_ref, dst_ref=buf, send_sem=ssem, recv_sem=rsem, device_id=peer, device_id_type=MESH)
    copy.start()
    o_ref[pl.ds(pl.multiple_of(tp * rows, rows), rows), :] = x_ref[...]
    copy.wait()
    o_ref[pl.ds(pl.multiple_of((1 - tp) * rows, rows), rows), :] = buf[...]


def swap_rows(x):
    rows, cols = x.shape
    return pl.pallas_call(
        swap_kernel,
        out_shape=jax.ShapeDtypeStruct((2 * rows, cols), x.dtype),
        in_specs=[pl.BlockSpec(memory_space=pltpu.VMEM)],
        out_specs=pl.BlockSpec(memory_space=pltpu.VMEM),
        scratch_shapes=[pltpu.VMEM((rows, cols), x.dtype), pltpu.SemaphoreType.DMA, pltpu.SemaphoreType.DMA],
        compiler_params=pltpu.CompilerParams(collective_id=1, has_side_effects=True),
        name='swap_rows',
    )(x)


def ring_step(i):
    return 1 + 2 * i - 3 * (i // 2)


def attn_kernel(scale2, q_ref, kt_ref, v_ref, x_ref, wo_hbm, h_ref, qb, kb, vb, so, ob, wo, part, jb, acc_s, m_s, l_s,
                wo_sem, q_ss, k_ss, v_ss, o_ss, q_rs, kx_rs, vx_rs, o_rs, k_rs, v_rs, kp_rs, vp_rs, kd_ss, vd_ss, kf_ss, vf_ss, kp_ss, vp_ss, j_ss, j_rs):
    cp, c = lax.axis_index('cp'), lax.axis_index('tp')
    x, y, z = cp % 4, (cp // 4) % 4, cp // 16
    g = z * 4 + y
    seg = kt_ref.shape[-1]
    half = seg // 2
    heads = qb.shape[0]

    def dev(xx, yy, zz, t):
        return (0, (zz % 4) * 16 + (yy % 4) * 4 + xx % 4, t)

    barrier = pltpu.get_barrier_semaphore()
    for d in STEPS:
        for t in range(2):
            pl.semaphore_signal(barrier, inc=1, device_id=dev(x + d, y, z, t), device_id_type=MESH)
        pl.semaphore_signal(barrier, inc=1, device_id=dev(x, y + d, z, c), device_id_type=MESH)
        pl.semaphore_signal(barrier, inc=1, device_id=dev(x, y, z + d, c), device_id_type=MESH)
    pl.semaphore_signal(barrier, inc=1, device_id=dev(x, y, z, 1 - c), device_id_type=MESH)
    wo_loads = [pltpu.make_async_copy(wo_hbm.at[:, hh], wo.at[hh], wo_sem.at[hh]) for hh in range(heads)]
    for copy in wo_loads:
        copy.start()
    pl.semaphore_wait(barrier, 13)

    def move(src, dst, ssem, rsem, xx, t, start):
        here = (xx == x) & (t == c)
        far = pltpu.make_async_remote_copy(src_ref=src, dst_ref=dst, send_sem=ssem, recv_sem=rsem, device_id=dev(xx, y, z, t), device_id_type=MESH)

        @pl.when(jnp.logical_not(here))
        def _():
            if start:
                far.start()
            else:
                far.wait_send()

        if start:
            @pl.when(here)
            def _():
                pltpu.make_async_copy(src, dst, rsem).start()

    def exchange(start):
        for j in range(2):
            for t in range(2):
                i = j * 2 + t
                move(kt_ref.at[j, t], kb.at[t, g, x], k_ss.at[i], kx_rs, 2 * c + j, t, start)
                move(v_ref.at[j, t], vb.at[t, g, x], v_ss.at[i], vx_rs, 2 * c + j, t, start)
        for hh in range(heads):
            for j in range(2):
                for t in range(2):
                    i = j * 2 + t
                    move(q_ref.at[:, pl.ds((i * heads + hh) * 128, 128)], qb.at[hh, x], q_ss.at[hh, i], q_rs.at[hh], 2 * c + j, t, start)

    def arrived(ref, sem):
        pltpu.make_async_copy(ref, ref, sem).wait()

    def push(buf, gg, yy, zz, t, ssem, rsem):
        pltpu.make_async_remote_copy(src_ref=buf.at[c, gg], dst_ref=buf.at[c, gg], send_sem=ssem, recv_sem=rsem.at[gg], device_id=dev(x, yy, zz, t), device_id_type=MESH).start()

    def to_partner(gg):
        push(kb, gg, y, z, 1 - c, kp_ss, kp_rs)
        push(vb, gg, y, z, 1 - c, vp_ss, vp_rs)

    def group(dy, dz):
        return ((z + 4 - dz) % 4) * 4 + (y + 4 - dy) % 4

    def pass_direct(i):
        d = ring_step(i)
        gy, gz = group(d, 0), group(0, d)
        for gg in (gy, gz):
            arrived(kb.at[c, gg], k_rs.at[gg])
            arrived(vb.at[c, gg], v_rs.at[gg])
        for e in STEPS:
            push(kb, gy, y, z + e, c, kf_ss, k_rs)
            push(vb, gz, y + e, z, c, vf_ss, v_rs)
        to_partner(gy)
        to_partner(gz)

    exchange(True)
    arrived(kb.at[c, g], kx_rs)
    arrived(vb.at[c, g], vx_rs)
    for d in STEPS:
        push(kb, g, y + d, z, c, kd_ss, k_rs)
        push(vb, g, y + d, z, c, vd_ss, v_rs)
        push(kb, g, y, z + d, c, kd_ss, k_rs)
        push(vb, g, y, z + d, c, vd_ss, v_rs)
        if d == 1:
            to_partner(g)

    keys = 4 * seg
    rows = 2 * seg

    def q_unit(qs, hh, xp):
        parts = [qb[hh, xx, pl.ds(pl.multiple_of(t * seg + qs * half, half), half), :] for xx in (2 * xp, 2 * xp + 1) for t in range(2)]
        return jnp.concatenate(parts, axis=0)

    def tiles(todo):
        def score(item):
            gg, qs, h, masked, first, hh, xp = item
            kt = jnp.concatenate([kb[h, gg, i] for i in range(4)], axis=1)
            return jnp.dot(q_unit(qs, hh, xp), kt, preferred_element_type=jnp.float32)

        s_next = score(todo[0])
        for n, (gg, qs, h, masked, first, hh, xp) in enumerate(todo):
            s = s_next
            if n + 1 < len(todo):
                s_next = score(todo[n + 1])
            if masked:
                col = lax.broadcasted_iota(jnp.int32, (rows, keys), 1)
                row = lax.broadcasted_iota(jnp.int32, (rows, keys), 0) + xp * rows
                ck, cq = col // seg, row // seg
                before = (ck < cq) if h == 0 else (ck > cq)
                s = jnp.where(before | ((ck == cq) & (col % seg <= row % seg)), s, NEG)
            at = pl.ds(xp * rows, rows)
            m_new = jnp.broadcast_to(jnp.max(s, axis=1, keepdims=True) * scale2, (rows, 128))
            if not first:
                m_prev = m_s[qs, hh, at]
                m_new = jnp.maximum(m_prev, m_new)
                alpha = jnp.exp2(m_prev - m_new)
            m_s[qs, hh, at] = m_new
            ps = [jnp.exp2(s[:, i * 128:(i + 1) * 128] * scale2 - m_new) for i in range(4)]
            lp = (ps[0] + ps[1]) + (ps[2] + ps[3])
            p = jnp.concatenate([v.astype(jnp.bfloat16) for v in ps], axis=1)
            pv = jnp.dot(p, vb[h, gg].reshape(keys, 128), preferred_element_type=jnp.float32)
            if first:
                l_s[qs, hh, at] = lp
                acc_s[qs, hh, at] = pv
            else:
                l_s[qs, hh, at] = l_s[qs, hh, at] * alpha + lp
                acc_s[qs, hh, at] = acc_s[qs, hh, at] * alpha + pv

    def ready(gg):
        arrived(kb.at[1 - c, gg], kp_rs.at[gg])
        arrived(vb.at[1 - c, gg], vp_rs.at[gg])

    def later(gg, hh):
        h = (gg > g).astype(jnp.int32)
        return [(gg, qs, hf, False, False, hh, xp) for qs, hf in ((1, 0), (h, h)) for xp in range(2)]

    def corner(i):
        return group(ring_step(i // 3), ring_step(i % 3))

    def pass_corner(i):
        gg = corner(i)
        arrived(kb.at[c, gg], k_rs.at[gg])
        arrived(vb.at[c, gg], v_rs.at[gg])
        to_partner(gg)

    pass_direct(0)
    ready(g)
    near = [group(1, 0), group(0, 1), group(3, 0), group(0, 3)]

    def first_phase(hh, _):
        arrived(qb.at[hh], q_rs.at[hh])
        tiles([(g, qs, hf, masked, first, hh, xp) for qs, hf, masked, first in ((1, 0, False, True), (0, 0, True, True), (1, 1, True, False)) for xp in range(2)])

        @pl.when(hh == 0)
        def _():
            pass_direct(1)
            for gg in near:
                ready(gg)

        @pl.when(hh == 1)
        def _():
            pass_direct(2)

        tiles([u for gg in near for u in later(gg, hh)])
        return 0

    lax.fori_loop(0, heads, first_phase, 0)

    for gg in (group(2, 0), group(0, 2)):
        ready(gg)
    pass_corner(0)

    def second_phase(i, _):
        gg_far = corner(jnp.maximum(i - 2, 0))
        gg = jnp.where(i == 0, group(2, 0), jnp.where(i == 1, group(0, 2), gg_far))

        @pl.when(i >= 1)
        def _():
            pass_corner(i)

        @pl.when(i >= 2)
        def _():
            ready(gg)

        tiles([u for hh in range(heads) for u in later(gg, hh)])
        return 0

    lax.fori_loop(0, 7, second_phase, 0)

    pass_corner(7)
    pass_corner(8)
    last = [corner(i) for i in range(5, 9)]
    for gg in last:
        ready(gg)

    def o_move(hh, start):
        for i in range(4):
            move(so.at[hh, i], ob.at[hh, (x % 2) * 2 + c], o_ss.at[hh, i], o_rs.at[hh], i, x // 2, start)

    def third_phase(hh, _):
        tiles([u for gg in last for u in later(gg, hh)])
        for qs in range(2):
            for xp in range(2):
                at = pl.ds(xp * rows, rows)
                out = (acc_s[qs, hh, at] / jnp.sum(l_s[qs, hh, at], axis=1, keepdims=True)).astype(so.dtype)
                for n, (xx, t) in enumerate([(xx, t) for xx in (2 * xp, 2 * xp + 1) for t in range(2)]):
                    so[hh, xx, t * seg + qs * half:t * seg + (qs + 1) * half, :] = out[n * half:(n + 1) * half]
        o_move(hh, True)
        return 0

    lax.fori_loop(0, heads, third_phase, 0)

    n_blk = 4
    wide = part.shape[1] // n_blk
    away = pl.ds(pl.multiple_of((1 - c) * seg, seg), seg)
    home = pl.ds(pl.multiple_of(c * seg, seg), seg)

    def cols(b):
        return pl.ds(b * wide, wide)

    def joined(b):
        return pltpu.make_async_remote_copy(src_ref=part.at[away, cols(b)], dst_ref=jb.at[:, cols(b)], send_sem=j_ss.at[b], recv_sem=j_rs.at[b], device_id=dev(x, y, z, 1 - c), device_id_type=MESH)

    for hh in range(heads):
        wo_loads[hh].wait()
        arrived(ob.at[hh], o_rs.at[hh])
        o_rows = jnp.concatenate([ob[hh, i] for i in range(4)], axis=1)
        for b in range(n_blk):
            term = jnp.dot(o_rows, wo[hh, :, :, b * wide:(b + 1) * wide].reshape(4 * 128, wide), preferred_element_type=jnp.float32)
            part[:, b * wide:(b + 1) * wide] = term if hh == 0 else part[:, b * wide:(b + 1) * wide] + term
            if hh == heads - 1:
                joined(b).start()
    for b in range(n_blk):
        joined(b).wait()
        at = slice(b * wide, (b + 1) * wide)
        h_ref[:, at] = (x_ref[:, at].astype(jnp.float32) + (part[home, at] + jb[:, at])).astype(h_ref.dtype)

    exchange(False)
    for hh in range(heads):
        o_move(hh, False)
    arrived(kb.at[0, pl.ds(0, 6)], kd_ss)
    arrived(vb.at[0, pl.ds(0, 6)], vd_ss)
    arrived(kb.at[0, pl.ds(0, 9)], kf_ss)
    arrived(vb.at[0, pl.ds(0, 9)], vf_ss)
    arrived(kb.at[0], kp_ss)
    arrived(vb.at[0], vp_ss)


def attention(q, kt, val, x_blk, w_o):
    rows, cols = q.shape
    seg = kt.shape[-1]
    heads = cols // 512
    d_model = x_blk.shape[1]
    dma = pltpu.SemaphoreType.DMA
    bf, f32 = jnp.bfloat16, jnp.float32
    vm = pl.BlockSpec(memory_space=pltpu.VMEM)
    return pl.pallas_call(
        functools.partial(attn_kernel, (128 ** -0.5) * math.log2(math.e)),
        out_shape=jax.ShapeDtypeStruct(x_blk.shape, bf),
        in_specs=[vm] * 4 + [pl.BlockSpec(memory_space=pltpu.HBM)],
        out_specs=vm,
        scratch_shapes=[
            pltpu.VMEM((heads, 4, rows, 128), bf),
            pltpu.VMEM((2, 16, 4, seg, 128), bf),
            pltpu.VMEM((2, 16, 4, seg, 128), bf),
            pltpu.VMEM((heads, 4, rows, 128), bf),
            pltpu.VMEM((heads, 4, rows, 128), bf),
            pltpu.VMEM((heads, 4, 128, d_model), bf),
            pltpu.VMEM((rows, d_model), f32),
            pltpu.VMEM(x_blk.shape, f32),
            pltpu.VMEM((2, heads, 4 * seg, 128), f32),
            pltpu.VMEM((2, heads, 4 * seg, 128), f32),
            pltpu.VMEM((2, heads, 4 * seg, 128), f32),
            dma((heads,)), dma((heads, 4)), dma((4,)), dma((4,)), dma((heads, 4)),
            dma((heads,)), dma, dma, dma((heads,)),
            dma((16,)), dma((16,)), dma((16,)), dma((16,)),
            dma, dma, dma, dma, dma, dma, dma((4,)), dma((4,)),
        ],
        compiler_params=pltpu.CompilerParams(collective_id=3, has_side_effects=True, vmem_limit_bytes=56 * 1024 * 1024),
        name='ring_attention',
    )(q, kt, val, x_blk, w_o.reshape(4, heads, 128, d_model))


def moe_kernel(h_ref, st_ref, s_ref, g_ref, wg_hbm, wu_hbm, wd_hbm, y_ref, send, recv, res, back, wg, wu, wd, w_sem, hop, s_ss, s_rs, r_ss, r_rs):
    cp, tp = lax.axis_index('cp'), lax.axis_index('tp')
    me = cp * 2 + tp
    x, y, z = cp % 4, (cp // 4) % 4, cp // 16
    n_dev, cap, width = send.shape
    n_grp = s_rs.shape[0]
    per = n_dev // n_grp
    rows = per * cap

    def dev(xx, yy, zz, t):
        return (0, (zz % 4) * 16 + (yy % 4) * 4 + xx % 4, t)

    loads = [pltpu.make_async_copy(a, b, w_sem.at[i]) for i, (a, b) in enumerate(((wg_hbm, wg), (wu_hbm, wu), (wd_hbm, wd)))]
    for copy in loads:
        copy.start()
    barrier = pltpu.get_barrier_semaphore()
    for d in STEPS:
        pl.semaphore_signal(barrier, inc=1, device_id=dev(x + d, y, z, tp), device_id_type=MESH)
        pl.semaphore_signal(barrier, inc=1, device_id=dev(x, y + d, z, tp), device_id_type=MESH)
        pl.semaphore_signal(barrier, inc=1, device_id=dev(x, y, z + d, tp), device_id_type=MESH)
    pl.semaphore_signal(barrier, inc=1, device_id=dev(x, y, z, 1 - tp), device_id_type=MESH)

    def pack(lo):
        at = lax.broadcasted_iota(jnp.int32, (rows, st_ref.shape[1]), 0) + lo * rows
        pick = (at == st_ref[0:1, :]) | (at == st_ref[1:2, :])
        out = jnp.dot(pick.astype(jnp.bfloat16), h_ref[...], preferred_element_type=jnp.float32)
        send[pl.ds(lo * per, per)] = out.astype(jnp.bfloat16).reshape(per, cap, width)

    for lo in range(n_grp):
        pack(lo)

    pl.semaphore_wait(barrier, 10)
    for d in STEPS:
        pl.semaphore_signal(hop.at[0], inc=1, device_id=dev(x, y + d, z, tp), device_id_type=MESH)
    pl.semaphore_wait(hop.at[0], 3)
    for d in STEPS:
        pl.semaphore_signal(hop.at[1], inc=1, device_id=dev(x, y, z + d, tp), device_id_type=MESH)
    pl.semaphore_wait(hop.at[1], 3)
    pl.semaphore_signal(hop.at[2], inc=1, device_id=dev(x, y, z, 1 - tp), device_id_type=MESH)
    pl.semaphore_wait(hop.at[2], 1)

    def peer(k, sign):
        j = (k * 91) % n_dev
        xx = (x + sign * ((j // 2) % 4)) % 4
        yy = (y + sign * ((j // 8) % 4)) % 4
        zz = (z + sign * (j // 32)) % 4
        return zz * 16 + yy * 4 + xx, (tp + j) % 2

    def give(k, _):
        c, t = peer(k, 1)
        pltpu.make_async_remote_copy(src_ref=send.at[c * 2 + t], dst_ref=recv.at[k], send_sem=s_ss, recv_sem=s_rs.at[k // per], device_id=(0, c, t), device_id_type=MESH).start()
        return 0

    own = pltpu.make_async_copy(send.at[me], recv.at[0], s_rs.at[0])
    own.start()
    lax.fori_loop(1, n_dev, give, 0)
    for copy in loads:
        copy.wait()

    def answer(k, _):
        c, t = peer(k, 3)
        pltpu.make_async_remote_copy(src_ref=res.at[k], dst_ref=back.at[me], send_sem=r_ss, recv_sem=r_rs, device_id=(0, c, t), device_id_type=MESH).start()
        return 0

    def group(i, _):
        part = recv.at[pl.ds(i * per, per)]
        pltpu.make_async_copy(part, part, s_rs.at[i]).wait()
        rows_in = part[...].reshape(rows, width)
        gate = jnp.dot(rows_in, wg[...], preferred_element_type=jnp.float32)
        up = jnp.dot(rows_in, wu[...], preferred_element_type=jnp.float32)
        act = (jax.nn.silu(gate) * up).astype(jnp.bfloat16)
        out = jnp.dot(act, wd[...], preferred_element_type=jnp.float32)
        res[pl.ds(i * per, per)] = out.astype(jnp.bfloat16).reshape(per, cap, width)
        lax.fori_loop(jnp.maximum(i * per, 1), (i + 1) * per, answer, 0)
        return 0

    lax.fori_loop(0, n_grp, group, 0)
    own_back = pltpu.make_async_copy(res.at[0], back.at[me], r_rs)
    own_back.start()
    pltpu.make_async_copy(back, back, r_rs).wait()
    all_back = back[...].reshape(n_dev * cap, width)
    at = lax.broadcasted_iota(jnp.int32, (s_ref.shape[0], n_dev * cap), 1)
    total = h_ref[...].astype(jnp.float32)
    moe = None
    for j in range(2):
        pick = (at == s_ref[:, j:j + 1]).astype(jnp.bfloat16)
        term = g_ref[:, j:j + 1] * jnp.dot(pick, all_back, preferred_element_type=jnp.float32)
        moe = term if moe is None else moe + term
    y_ref[...] = (total + moe).astype(y_ref.dtype)
    most = send.at[pl.ds(1, n_dev - 1)]
    pltpu.make_async_copy(most, most, s_ss).wait()
    pltpu.make_async_copy(most, most, r_ss).wait()


def moe(hidden, slot_ids, gates, w_gate, w_up, w_down, cap):
    d_model, ff = w_gate.shape
    n_dev = 4 * hidden.shape[0] // cap
    dma = pltpu.SemaphoreType.DMA
    bf = jnp.bfloat16
    vm = pl.BlockSpec(memory_space=pltpu.VMEM)
    anyspace = pl.BlockSpec(memory_space=pltpu.HBM)
    buf = pltpu.VMEM((n_dev, cap, d_model), bf)
    n_grp = 4
    return pl.pallas_call(
        moe_kernel,
        out_shape=jax.ShapeDtypeStruct(hidden.shape, bf),
        in_specs=[vm] * 4 + [anyspace] * 3,
        out_specs=vm,
        scratch_shapes=[
            buf, buf, buf, buf,
            pltpu.VMEM((d_model, ff), bf), pltpu.VMEM((d_model, ff), bf), pltpu.VMEM((ff, d_model), bf),
            dma((3,)), pltpu.SemaphoreType.REGULAR((3,)), dma, dma((n_grp,)), dma, dma,
        ],
        compiler_params=pltpu.CompilerParams(collective_id=4, has_side_effects=True, vmem_limit_bytes=48 * 1024 * 1024),
        name='moe_exchange',
    )(hidden, slot_ids.T, slot_ids, gates, w_gate, w_up, w_down)


def solution(mesh):
    cp_size = mesh.shape['cp']
    tp_size = mesh.shape['tp']
    num_devs = cp_size * tp_size
    row_spec = P(('data', 'cp', 'tp'), None)
    head_spec = P(None, 'tp', None)
    wo_spec = P('tp', None, None)
    expert_spec = P(('cp', 'tp'), None, None)

    def device_fn(x_blk, w_q, w_k, w_v, w_o, idx_blk, gate_blk, w_gate, w_up, w_down):
        tok_dev, d_model = x_blk.shape
        half = tok_dev // 2
        exp_local = w_gate.shape[0]
        num_exp = exp_local * num_devs
        capacity = 4 * tok_dev // num_exp

        x_rows = swap_rows(x_blk)
        x_seg = x_rows.reshape(2, 2, half, d_model).swapaxes(0, 1).reshape(2, tok_dev, d_model)
        key_t = jnp.einsum('mnc,hsm->nhcs', w_k, x_seg, preferred_element_type=jnp.float32).astype(jnp.bfloat16)
        val = jnp.einsum('hsm,mnc->nhsc', x_seg, w_v, preferred_element_type=jnp.float32).astype(jnp.bfloat16)
        queries = jnp.dot(x_rows, w_q.reshape(d_model, -1), preferred_element_type=jnp.float32).astype(jnp.bfloat16)
        hidden = attention(queries, key_t, val, x_blk, w_o)

        flat_ids = idx_blk.reshape(-1)
        onehot = (flat_ids[:, None] == jnp.arange(num_exp)[None, :]).astype(jnp.int32)
        slot_pos = jnp.sum(jnp.cumsum(onehot, axis=0) * onehot, axis=1) - 1
        slot_ids = (flat_ids * capacity + slot_pos).reshape(tok_dev, 2)
        return moe(hidden, slot_ids, gate_blk, w_gate[0], w_up[0], w_down[0], capacity)

    return jax.shard_map(device_fn, mesh=mesh, in_specs=(row_spec, head_spec, head_spec, head_spec, wo_spec, row_spec, row_spec, expert_spec, expert_spec, expert_spec), out_specs=row_spec, check_vma=False)
```

```python
import functools
import math

import jax
import jax.numpy as jnp
from jax import lax
from jax.experimental import pallas as pl
from jax.experimental.pallas import tpu as pltpu
from jax.sharding import PartitionSpec as P

NEG = -1e30
MESH = pl.DeviceIdType.MESH
STEPS = (1, 3, 2)


def swap_kernel(x_ref, o_ref, buf, ssem, rsem):
    cp, tp = lax.axis_index('cp'), lax.axis_index('tp')
    peer = (0, cp, 1 - tp)
    rows = x_ref.shape[0]
    barrier = pltpu.get_barrier_semaphore()
    pl.semaphore_signal(barrier, inc=1, device_id=peer, device_id_type=MESH)
    pl.semaphore_wait(barrier, 1)
    copy = pltpu.make_async_remote_copy(src_ref=x_ref, dst_ref=buf, send_sem=ssem, recv_sem=rsem, device_id=peer, device_id_type=MESH)
    copy.start()
    half = rows // 2

    def put(src, t):
        for h in range(2):
            o_ref[pl.ds(pl.multiple_of(h * rows + t * half, half), half), :] = src[h * half:(h + 1) * half]

    put(x_ref, tp)
    copy.wait()
    put(buf, 1 - tp)


def swap_rows(x):
    rows, cols = x.shape
    return pl.pallas_call(
        swap_kernel,
        out_shape=jax.ShapeDtypeStruct((2 * rows, cols), x.dtype),
        in_specs=[pl.BlockSpec(memory_space=pltpu.VMEM)],
        out_specs=pl.BlockSpec(memory_space=pltpu.VMEM),
        scratch_shapes=[pltpu.VMEM((rows, cols), x.dtype), pltpu.SemaphoreType.DMA, pltpu.SemaphoreType.DMA],
        compiler_params=pltpu.CompilerParams(collective_id=1, has_side_effects=True),
        name='swap_rows',
    )(x)


def ring_step(i):
    return 1 + 2 * i - 3 * (i // 2)


def block_kernel(scale2, q_ref, kt_ref, v_ref, x_ref, st_ref, s_ref, g_ref, wo_hbm, wg_hbm, wu_hbm, wd_hbm, y_ref, qb, kb, vb, so, ob, wo, part, jb, acc_s, m_s, l_s,
                 h_ref, send, recv, res, back, wg, wu, wd, w_sem, hop, s_ss, s_rs, r_ss, r_rs,
                 wo_sem, q_ss, k_ss, v_ss, o_ss, q_rs, kx_rs, vx_rs, o_rs, k_rs, v_rs, kp_rs, vp_rs, kd_ss, vd_ss, kf_ss, vf_ss, kp_ss, vp_ss, j_ss, j_rs):
    cp, c = lax.axis_index('cp'), lax.axis_index('tp')
    x, y, z = cp % 4, (cp // 4) % 4, cp // 16
    g = z * 4 + y
    seg = kt_ref.shape[-1]
    half = seg // 2
    heads = qb.shape[0]
    me = cp * 2 + c

    def dev(xx, yy, zz, t):
        return (0, (zz % 4) * 16 + (yy % 4) * 4 + xx % 4, t)

    barrier = pltpu.get_barrier_semaphore()
    for d in STEPS:
        for t in range(2):
            pl.semaphore_signal(barrier, inc=1, device_id=dev(x + d, y, z, t), device_id_type=MESH)
        pl.semaphore_signal(barrier, inc=1, device_id=dev(x, y + d, z, c), device_id_type=MESH)
        pl.semaphore_signal(barrier, inc=1, device_id=dev(x, y, z + d, c), device_id_type=MESH)
    pl.semaphore_signal(barrier, inc=1, device_id=dev(x, y, z, 1 - c), device_id_type=MESH)
    wo_loads = [pltpu.make_async_copy(wo_hbm.at[:, hh], wo.at[hh], wo_sem.at[hh]) for hh in range(heads)]
    for copy in wo_loads:
        copy.start()
    loads = [pltpu.make_async_copy(a, b, w_sem.at[i]) for i, (a, b) in enumerate(((wg_hbm, wg), (wu_hbm, wu), (wd_hbm, wd)))]
    for copy in loads:
        copy.start()
    pl.semaphore_wait(barrier, 13)
    for d in STEPS:
        pl.semaphore_signal(hop.at[0], inc=1, device_id=dev(x, y + d, z, c), device_id_type=MESH)

    def move(src, dst, ssem, rsem, xx, t, start):
        here = (xx == x) & (t == c)
        far = pltpu.make_async_remote_copy(src_ref=src, dst_ref=dst, send_sem=ssem, recv_sem=rsem, device_id=dev(xx, y, z, t), device_id_type=MESH)

        @pl.when(jnp.logical_not(here))
        def _():
            if start:
                far.start()
            else:
                far.wait_send()

        if start:
            @pl.when(here)
            def _():
                pltpu.make_async_copy(src, dst, rsem).start()

    def exchange(start):
        for j in range(2):
            for t in range(2):
                i = j * 2 + t
                move(kt_ref.at[j, t], kb.at[t, g, x], k_ss.at[i], kx_rs, 2 * c + j, t, start)
                move(v_ref.at[j, t], vb.at[t, g, x], v_ss.at[i], vx_rs, 2 * c + j, t, start)
        for hh in range(heads):
            for j in range(2):
                for t in range(2):
                    i = j * 2 + t
                    move(q_ref.at[:, pl.ds((i * heads + hh) * 128, 128)], qb.at[hh, x], q_ss.at[hh, i], q_rs.at[hh], 2 * c + j, t, start)

    def arrived(ref, sem):
        pltpu.make_async_copy(ref, ref, sem).wait()

    def push(buf, gg, yy, zz, t, ssem, rsem):
        pltpu.make_async_remote_copy(src_ref=buf.at[c, gg], dst_ref=buf.at[c, gg], send_sem=ssem, recv_sem=rsem.at[gg], device_id=dev(x, yy, zz, t), device_id_type=MESH).start()

    def to_partner(gg):
        push(kb, gg, y, z, 1 - c, kp_ss, kp_rs)
        push(vb, gg, y, z, 1 - c, vp_ss, vp_rs)

    def group(dy, dz):
        return ((z + 4 - dz) % 4) * 4 + (y + 4 - dy) % 4

    def pass_direct(i):
        d = ring_step(i)
        gy, gz = group(d, 0), group(0, d)
        for gg in (gy, gz):
            arrived(kb.at[c, gg], k_rs.at[gg])
            arrived(vb.at[c, gg], v_rs.at[gg])
        for e in STEPS:
            push(kb, gy, y, z + e, c, kf_ss, k_rs)
            push(vb, gz, y + e, z, c, vf_ss, v_rs)
        to_partner(gy)
        to_partner(gz)

    exchange(True)
    arrived(kb.at[c, g], kx_rs)
    arrived(vb.at[c, g], vx_rs)
    for d in STEPS:
        push(kb, g, y + d, z, c, kd_ss, k_rs)
        push(vb, g, y + d, z, c, vd_ss, v_rs)
        push(kb, g, y, z + d, c, kd_ss, k_rs)
        push(vb, g, y, z + d, c, vd_ss, v_rs)
        if d == 1:
            to_partner(g)

    rows = 2 * seg

    def q_unit(qs, hh, xp):
        parts = [qb[hh, xx, pl.ds(pl.multiple_of(qs * seg, seg), seg), :] for xx in (2 * xp, 2 * xp + 1)]
        return jnp.concatenate(parts, axis=0)

    def tiles(todo):
        def score(item):
            ggs, qs, h, masked, first, hh, xp = item
            kt = jnp.concatenate([kb[h, gg, i] for gg in ggs for i in range(4)], axis=1)
            return jnp.dot(q_unit(qs, hh, xp), kt, preferred_element_type=jnp.float32)

        s_next = score(todo[0])
        for n, (ggs, qs, h, masked, first, hh, xp) in enumerate(todo):
            s = s_next
            keys = s.shape[1]
            if n + 1 < len(todo):
                s_next = score(todo[n + 1])
            if masked:
                col = lax.broadcasted_iota(jnp.int32, (rows, keys), 1)
                row = lax.broadcasted_iota(jnp.int32, (rows, keys), 0) + xp * rows
                ck, cq = col // seg, row // seg
                before = (ck < cq) if h == 0 else (ck > cq)
                s = jnp.where(before | ((ck == cq) & (col % seg <= row % seg)), s, NEG)
            at = pl.ds(xp * rows, rows)
            m_new = jnp.broadcast_to(jnp.max(s, axis=1, keepdims=True) * scale2, (rows, 128))
            if not first:
                m_prev = m_s[qs, hh, at]
                m_new = jnp.maximum(m_prev, m_new)
                alpha = jnp.exp2(m_prev - m_new)
            m_s[qs, hh, at] = m_new
            ps = [jnp.exp2(s[:, i * 128:(i + 1) * 128] * scale2 - m_new) for i in range(keys // 128)]
            lp = ps[0]
            for v in ps[1:]:
                lp = lp + v
            p = jnp.concatenate([v.astype(jnp.bfloat16) for v in ps], axis=1)
            val = jnp.concatenate([vb[h, gg].reshape(4 * seg, 128) for gg in ggs], axis=0)
            pv = jnp.dot(p, val, preferred_element_type=jnp.float32)
            if first:
                l_s[qs, hh, at] = lp
                acc_s[qs, hh, at] = pv
            else:
                l_s[qs, hh, at] = l_s[qs, hh, at] * alpha + lp
                acc_s[qs, hh, at] = acc_s[qs, hh, at] * alpha + pv

    def ready(gg):
        arrived(kb.at[1 - c, gg], kp_rs.at[gg])
        arrived(vb.at[1 - c, gg], vp_rs.at[gg])

    def later(ggs, hh):
        todo = []
        for n in range(0, len(ggs), 2):
            pair = ggs[n:n + 2]
            todo += [(pair, 1, 0, False, False, hh, xp) for xp in range(2)]
            for gg in pair:
                h = (gg > g).astype(jnp.int32)
                todo += [([gg], h, h, False, False, hh, xp) for xp in range(2)]
        return todo

    def corner(i):
        return group(ring_step(i // 3), ring_step(i % 3))

    def pass_corner(i):
        gg = corner(i)
        arrived(kb.at[c, gg], k_rs.at[gg])
        arrived(vb.at[c, gg], v_rs.at[gg])
        to_partner(gg)

    pass_direct(0)
    pl.semaphore_wait(hop.at[0], 3)
    for d in STEPS:
        pl.semaphore_signal(hop.at[1], inc=1, device_id=dev(x, y, z + d, c), device_id_type=MESH)
    ready(g)
    near = [group(1, 0), group(0, 1), group(3, 0), group(0, 3)]

    def first_phase(hh, _):
        arrived(qb.at[hh], q_rs.at[hh])
        tiles([([g], qs, hf, masked, first, hh, xp) for qs, hf, masked, first in ((1, 0, False, True), (0, 0, True, True), (1, 1, True, False)) for xp in range(2)])

        @pl.when(hh == 0)
        def _():
            pass_direct(1)
            for gg in near:
                ready(gg)

        @pl.when(hh == 1)
        def _():
            pass_direct(2)

        tiles(later(near, hh))
        return 0

    lax.fori_loop(0, heads, first_phase, 0)

    pass_corner(0)
    pass_corner(1)

    def second_phase(i, _):
        first_c = corner(jnp.maximum(2 * i - 2, 0))
        second_c = corner(jnp.maximum(2 * i - 1, 0))
        pair = [jnp.where(i == 0, group(2, 0), first_c), jnp.where(i == 0, group(0, 2), second_c)]
        for gg in pair:
            ready(gg)
        tiles([u for hh in range(heads // 2) for u in later(pair, hh)])
        pass_corner(2 * i + 2)
        pass_corner(2 * i + 3)
        tiles([u for hh in range(heads // 2, heads) for u in later(pair, hh)])
        return 0

    lax.fori_loop(0, 3, second_phase, 0)

    pass_corner(8)
    last = [corner(i) for i in range(4, 9)]
    for gg in last:
        ready(gg)

    def o_move(hh, start):
        for i in range(4):
            move(so.at[hh, i], ob.at[hh, (x % 2) * 2 + c], o_ss.at[hh, i], o_rs.at[hh], i, x // 2, start)

    def third_phase(hh, _):
        tiles(later(last, hh))
        for qs in range(2):
            for xp in range(2):
                at = pl.ds(xp * rows, rows)
                out = (acc_s[qs, hh, at] / jnp.sum(l_s[qs, hh, at], axis=1, keepdims=True)).astype(so.dtype)
                for n in range(2):
                    so[hh, 2 * xp + n, qs * seg:(qs + 1) * seg, :] = out[n * seg:(n + 1) * seg]
        o_move(hh, True)
        return 0

    lax.fori_loop(0, heads, third_phase, 0)

    n_blk = 4
    wide = part.shape[3] // n_blk

    def cols(b):
        return pl.ds(b * wide, wide)

    def joined(b):
        return pltpu.make_async_remote_copy(src_ref=part.at[:, 1 - c, :, cols(b)], dst_ref=jb.at[:, :, cols(b)], send_sem=j_ss.at[b], recv_sem=j_rs.at[b], device_id=dev(x, y, z, 1 - c), device_id_type=MESH)

    for hh in range(heads):
        wo_loads[hh].wait()
        arrived(ob.at[hh], o_rs.at[hh])
        o_rows = jnp.concatenate([ob[hh, i] for i in range(4)], axis=1)
        for b in range(n_blk):
            term = jnp.dot(o_rows, wo[hh, :, :, b * wide:(b + 1) * wide].reshape(4 * 128, wide), preferred_element_type=jnp.float32)
            at = slice(b * wide, (b + 1) * wide)
            term = term.reshape(2, 2, half, wide)
            part[:, :, :, at] = term if hh == 0 else part[:, :, :, at] + term
            if hh == heads - 1:
                joined(b).start()
    for b in range(n_blk):
        joined(b).wait()
        at = slice(b * wide, (b + 1) * wide)
        for n in range(2):
            own_rows = slice(n * half, (n + 1) * half)
            h_ref[own_rows, at] = (x_ref[own_rows, at].astype(jnp.float32) + (part[n, c, :, at] + jb[n, :, at])).astype(h_ref.dtype)

    n_dev, cap, width = send.shape
    n_grp = s_rs.shape[0]
    per = n_dev // n_grp
    rows = per * cap
    for copy in loads:
        copy.wait()

    def pack(lo):
        at = lax.broadcasted_iota(jnp.int32, (seg, st_ref.shape[1]), 0) + lo * seg
        pick = (at == st_ref[0:1, :]) | (at == st_ref[1:2, :])
        out = jnp.dot(pick.astype(jnp.bfloat16), h_ref[...], preferred_element_type=jnp.float32)
        send[pl.ds(lo * (seg // cap), seg // cap)] = out.astype(jnp.bfloat16).reshape(seg // cap, cap, width)

    for lo in range(n_dev * cap // seg):
        pack(lo)

    pl.semaphore_wait(hop.at[1], 3)

    def peer(k, sign):
        j = (k * 91) % n_dev
        xx = (x + sign * ((j // 2) % 4)) % 4
        yy = (y + sign * ((j // 8) % 4)) % 4
        zz = (z + sign * (j // 32)) % 4
        return zz * 16 + yy * 4 + xx, (c + j) % 2

    def give(k, _):
        pc, t = peer(k, 1)
        pltpu.make_async_remote_copy(src_ref=send.at[pc * 2 + t], dst_ref=recv.at[k], send_sem=s_ss, recv_sem=s_rs.at[k // per], device_id=(0, pc, t), device_id_type=MESH).start()
        return 0

    own = pltpu.make_async_copy(send.at[me], recv.at[0], s_rs.at[0])
    own.start()
    lax.fori_loop(1, n_dev, give, 0)

    def answer(k, _):
        pc, t = peer(k, 3)
        pltpu.make_async_remote_copy(src_ref=res.at[k], dst_ref=back.at[me], send_sem=r_ss, recv_sem=r_rs, device_id=(0, pc, t), device_id_type=MESH).start()
        return 0

    def group(i, _):
        part = recv.at[pl.ds(i * per, per)]
        pltpu.make_async_copy(part, part, s_rs.at[i]).wait()
        rows_in = part[...].reshape(rows, width)
        gate = jnp.dot(rows_in, wg[...], preferred_element_type=jnp.float32)
        up = jnp.dot(rows_in, wu[...], preferred_element_type=jnp.float32)
        act = (jax.nn.silu(gate) * up).astype(jnp.bfloat16)
        out = jnp.dot(act, wd[...], preferred_element_type=jnp.float32)
        res[pl.ds(i * per, per)] = out.astype(jnp.bfloat16).reshape(per, cap, width)
        lax.fori_loop(jnp.maximum(i * per, 1), (i + 1) * per, answer, 0)
        return 0

    lax.fori_loop(0, n_grp, group, 0)
    own_back = pltpu.make_async_copy(res.at[0], back.at[me], r_rs)
    own_back.start()
    pltpu.make_async_copy(back, back, r_rs).wait()
    all_back = back[...].reshape(n_dev * cap, width)
    at = lax.broadcasted_iota(jnp.int32, (s_ref.shape[0], n_dev * cap), 1)
    total = h_ref[...].astype(jnp.float32)
    moe = None
    for j in range(2):
        pick = (at == s_ref[:, j:j + 1]).astype(jnp.bfloat16)
        term = g_ref[:, j:j + 1] * jnp.dot(pick, all_back, preferred_element_type=jnp.float32)
        moe = term if moe is None else moe + term
    y_ref[...] = (total + moe).astype(y_ref.dtype)
    most = send.at[pl.ds(1, n_dev - 1)]
    pltpu.make_async_copy(most, most, s_ss).wait()
    pltpu.make_async_copy(most, most, r_ss).wait()
    exchange(False)
    for hh in range(heads):
        o_move(hh, False)
    arrived(kb.at[0, pl.ds(0, 6)], kd_ss)
    arrived(vb.at[0, pl.ds(0, 6)], vd_ss)
    arrived(kb.at[0, pl.ds(0, 9)], kf_ss)
    arrived(vb.at[0, pl.ds(0, 9)], vf_ss)
    arrived(kb.at[0], kp_ss)
    arrived(vb.at[0], vp_ss)


def block(q, kt, val, x_blk, slot_ids, gates, w_o, w_gate, w_up, w_down, cap):
    rows, cols = q.shape
    seg = kt.shape[-1]
    heads = cols // 512
    tok_dev, d_model = x_blk.shape
    ff = w_gate.shape[1]
    n_dev = 4 * tok_dev // cap
    n_grp = 8
    dma = pltpu.SemaphoreType.DMA
    bf, f32 = jnp.bfloat16, jnp.float32
    vm = pl.BlockSpec(memory_space=pltpu.VMEM)
    hbm = pl.BlockSpec(memory_space=pltpu.HBM)
    buf = pltpu.VMEM((n_dev, cap, d_model), bf)
    return pl.pallas_call(
        functools.partial(block_kernel, (128 ** -0.5) * math.log2(math.e)),
        out_shape=jax.ShapeDtypeStruct(x_blk.shape, bf),
        in_specs=[vm] * 7 + [hbm] * 4,
        out_specs=vm,
        scratch_shapes=[
            pltpu.VMEM((heads, 4, rows, 128), bf),
            pltpu.VMEM((2, 16, 4, seg, 128), bf),
            pltpu.VMEM((2, 16, 4, seg, 128), bf),
            pltpu.VMEM((heads, 4, rows, 128), bf),
            pltpu.VMEM((heads, 4, rows, 128), bf),
            pltpu.VMEM((heads, 4, 128, d_model), bf),
            pltpu.VMEM((2, 2, tok_dev // 2, d_model), f32),
            pltpu.VMEM((2, tok_dev // 2, d_model), f32),
            pltpu.VMEM((2, heads, 4 * seg, 128), f32),
            pltpu.VMEM((2, heads, 4 * seg, 128), f32),
            pltpu.VMEM((2, heads, 4 * seg, 128), f32),
            pltpu.VMEM(x_blk.shape, bf),
            buf, buf, buf, buf,
            pltpu.VMEM((d_model, ff), bf), pltpu.VMEM((d_model, ff), bf), pltpu.VMEM((ff, d_model), bf),
            dma((3,)), pltpu.SemaphoreType.REGULAR((2,)), dma, dma((n_grp,)), dma, dma,
            dma((heads,)), dma((heads, 4)), dma((4,)), dma((4,)), dma((heads, 4)),
            dma((heads,)), dma, dma, dma((heads,)),
            dma((16,)), dma((16,)), dma((16,)), dma((16,)),
            dma, dma, dma, dma, dma, dma, dma((4,)), dma((4,)),
        ],
        compiler_params=pltpu.CompilerParams(collective_id=3, has_side_effects=True, vmem_limit_bytes=60 * 1024 * 1024),
        name='ring_block',
    )(q, kt, val, x_blk, slot_ids.T, slot_ids, gates, w_o.reshape(4, heads, 128, d_model), w_gate, w_up, w_down)


def solution(mesh):
    cp_size = mesh.shape['cp']
    tp_size = mesh.shape['tp']
    num_devs = cp_size * tp_size
    row_spec = P(('data', 'cp', 'tp'), None)
    head_spec = P(None, 'tp', None)
    wo_spec = P('tp', None, None)
    expert_spec = P(('cp', 'tp'), None, None)

    def device_fn(x_blk, w_q, w_k, w_v, w_o, idx_blk, gate_blk, w_gate, w_up, w_down):
        tok_dev, d_model = x_blk.shape
        exp_local = w_gate.shape[0]
        num_exp = exp_local * num_devs
        capacity = 4 * tok_dev // num_exp

        x_rows = swap_rows(x_blk)
        x_seg = x_rows.reshape(2, tok_dev, d_model)
        key_t = jnp.einsum('mnc,hsm->nhcs', w_k, x_seg, preferred_element_type=jnp.float32).astype(jnp.bfloat16)
        val = jnp.einsum('hsm,mnc->nhsc', x_seg, w_v, preferred_element_type=jnp.float32).astype(jnp.bfloat16)
        queries = jnp.dot(x_rows, w_q.reshape(d_model, -1), preferred_element_type=jnp.float32).astype(jnp.bfloat16)
        flat_ids = idx_blk.reshape(-1)
        onehot = (flat_ids[:, None] == jnp.arange(num_exp)[None, :]).astype(jnp.int32)
        slot_pos = jnp.sum(jnp.cumsum(onehot, axis=0) * onehot, axis=1) - 1
        slot_ids = (flat_ids * capacity + slot_pos).reshape(tok_dev, 2)
        return block(queries, key_t, val, x_blk, slot_ids, gate_blk, w_o, w_gate[0], w_up[0], w_down[0], capacity)

    return jax.shard_map(device_fn, mesh=mesh, in_specs=(row_spec, head_spec, head_spec, head_spec, wo_spec, row_spec, row_spec, expert_spec, expert_spec, expert_spec), out_specs=row_spec, check_vma=False)
```

```python
import functools
import math

import jax
import jax.numpy as jnp
from jax import lax
from jax.experimental import pallas as pl
from jax.experimental.pallas import tpu as pltpu
from jax.sharding import PartitionSpec as P

NEG = -1e30
MESH = pl.DeviceIdType.MESH
STEPS = (1, 3, 2)


def swap_kernel(x_ref, o_ref, buf, ssem, rsem):
    cp, tp = lax.axis_index('cp'), lax.axis_index('tp')
    peer = (0, cp, 1 - tp)
    rows = x_ref.shape[0]
    barrier = pltpu.get_barrier_semaphore()
    pl.semaphore_signal(barrier, inc=1, device_id=peer, device_id_type=MESH)
    pl.semaphore_wait(barrier, 1)
    copy = pltpu.make_async_remote_copy(src_ref=x_ref, dst_ref=buf, send_sem=ssem, recv_sem=rsem, device_id=peer, device_id_type=MESH)
    copy.start()
    half = rows // 2

    def put(src, t):
        for h in range(2):
            o_ref[pl.ds(pl.multiple_of(h * rows + t * half, half), half), :] = src[h * half:(h + 1) * half]

    put(x_ref, tp)
    copy.wait()
    put(buf, 1 - tp)


def swap_rows(x):
    rows, cols = x.shape
    return pl.pallas_call(
        swap_kernel,
        out_shape=jax.ShapeDtypeStruct((2 * rows, cols), x.dtype),
        in_specs=[pl.BlockSpec(memory_space=pltpu.VMEM)],
        out_specs=pl.BlockSpec(memory_space=pltpu.VMEM),
        scratch_shapes=[pltpu.VMEM((rows, cols), x.dtype), pltpu.SemaphoreType.DMA, pltpu.SemaphoreType.DMA],
        compiler_params=pltpu.CompilerParams(collective_id=1, has_side_effects=True),
        name='swap_rows',
    )(x)


def ring_step(i):
    return 1 + 2 * i - 3 * (i // 2)


def block_kernel(scale2, q_ref, kt_ref, v_ref, x_ref, st_ref, s_ref, g_ref, wo_hbm, wg_hbm, wu_hbm, wd_hbm, y_ref, qb, kb, vb, so, ob, wo, part, jb, acc_s, m_s, l_s,
                 h_ref, send, recv, res, back, wg, wu, wd, w_sem, hop, s_ss, s_rs, r_ss, r_rs,
                 wo_sem, q_ss, k_ss, v_ss, o_ss, q_rs, kx_rs, vx_rs, o_rs, k_rs, v_rs, kp_rs, vp_rs, kd_ss, vd_ss, kf_ss, vf_ss, kp_ss, vp_ss, j_ss, j_rs):
    cp, c = lax.axis_index('cp'), lax.axis_index('tp')
    x, y, z = cp % 4, (cp // 4) % 4, cp // 16
    g = z * 4 + y
    seg = kt_ref.shape[-1]
    half = seg // 2
    heads = qb.shape[0]
    me = cp * 2 + c

    def dev(xx, yy, zz, t):
        return (0, (zz % 4) * 16 + (yy % 4) * 4 + xx % 4, t)

    barrier = pltpu.get_barrier_semaphore()
    for d in STEPS:
        for t in range(2):
            pl.semaphore_signal(barrier, inc=1, device_id=dev(x + d, y, z, t), device_id_type=MESH)
        pl.semaphore_signal(barrier, inc=1, device_id=dev(x, y + d, z, c), device_id_type=MESH)
        pl.semaphore_signal(barrier, inc=1, device_id=dev(x, y, z + d, c), device_id_type=MESH)
    pl.semaphore_signal(barrier, inc=1, device_id=dev(x, y, z, 1 - c), device_id_type=MESH)
    wo_loads = [pltpu.make_async_copy(wo_hbm.at[:, hh], wo.at[hh], wo_sem.at[hh]) for hh in range(heads)]
    for copy in wo_loads:
        copy.start()
    loads = [pltpu.make_async_copy(a, b, w_sem.at[i]) for i, (a, b) in enumerate(((wg_hbm, wg), (wu_hbm, wu), (wd_hbm, wd)))]
    for copy in loads:
        copy.start()
    pl.semaphore_wait(barrier, 13)
    for d in STEPS:
        pl.semaphore_signal(hop.at[0], inc=1, device_id=dev(x, y + d, z, c), device_id_type=MESH)

    def move(src, dst, ssem, rsem, xx, t, start):
        here = (xx == x) & (t == c)
        far = pltpu.make_async_remote_copy(src_ref=src, dst_ref=dst, send_sem=ssem, recv_sem=rsem, device_id=dev(xx, y, z, t), device_id_type=MESH)

        @pl.when(jnp.logical_not(here))
        def _():
            if start:
                far.start()
            else:
                far.wait_send()

        if start:
            @pl.when(here)
            def _():
                pltpu.make_async_copy(src, dst, rsem).start()

    def exchange(start):
        for j in range(2):
            for t in range(2):
                i = j * 2 + t
                move(kt_ref.at[j, t], kb.at[t, g, x], k_ss.at[i], kx_rs, 2 * c + j, t, start)
                move(v_ref.at[j, t], vb.at[t, g, x], v_ss.at[i], vx_rs, 2 * c + j, t, start)
        for hh in range(heads):
            for j in range(2):
                for t in range(2):
                    i = j * 2 + t
                    move(q_ref.at[:, pl.ds((i * heads + hh) * 128, 128)], qb.at[hh, x], q_ss.at[hh, i], q_rs.at[hh], 2 * c + j, t, start)

    def arrived(ref, sem):
        pltpu.make_async_copy(ref, ref, sem).wait()

    def push(buf, gg, yy, zz, t, ssem, rsem):
        pltpu.make_async_remote_copy(src_ref=buf.at[c, gg], dst_ref=buf.at[c, gg], send_sem=ssem, recv_sem=rsem.at[gg], device_id=dev(x, yy, zz, t), device_id_type=MESH).start()

    def to_partner(gg):
        push(kb, gg, y, z, 1 - c, kp_ss, kp_rs)
        push(vb, gg, y, z, 1 - c, vp_ss, vp_rs)

    def group(dy, dz):
        return ((z + 4 - dz) % 4) * 4 + (y + 4 - dy) % 4

    def pass_direct(i):
        d = ring_step(i)
        gy, gz = group(d, 0), group(0, d)
        for gg in (gy, gz):
            arrived(kb.at[c, gg], k_rs.at[gg])
            arrived(vb.at[c, gg], v_rs.at[gg])
        for e in STEPS:
            push(kb, gy, y, z + e, c, kf_ss, k_rs)
            push(vb, gz, y + e, z, c, vf_ss, v_rs)
        to_partner(gy)
        to_partner(gz)

    exchange(True)
    arrived(kb.at[c, g], kx_rs)
    arrived(vb.at[c, g], vx_rs)
    for d in STEPS:
        push(kb, g, y + d, z, c, kd_ss, k_rs)
        push(vb, g, y + d, z, c, vd_ss, v_rs)
        push(kb, g, y, z + d, c, kd_ss, k_rs)
        push(vb, g, y, z + d, c, vd_ss, v_rs)
        if d == 1:
            to_partner(g)

    rows = 2 * seg

    def q_unit(qs, hh, xp):
        parts = [qb[hh, xx, pl.ds(pl.multiple_of(qs * seg, seg), seg), :] for xx in (2 * xp, 2 * xp + 1)]
        return jnp.concatenate(parts, axis=0)

    def tiles(todo):
        def score(item):
            ggs, qs, h, masked, first, hh, xp = item
            kt = jnp.concatenate([kb[h, gg, i] for gg in ggs for i in range(4)], axis=1)
            return jnp.dot(q_unit(qs, hh, xp), kt, preferred_element_type=jnp.float32)

        s_next = score(todo[0])
        for n, (ggs, qs, h, masked, first, hh, xp) in enumerate(todo):
            s = s_next
            keys = s.shape[1]
            if n + 1 < len(todo):
                s_next = score(todo[n + 1])
            if masked:
                col = lax.broadcasted_iota(jnp.int32, (rows, keys), 1)
                row = lax.broadcasted_iota(jnp.int32, (rows, keys), 0) + xp * rows
                ck, cq = col // seg, row // seg
                before = (ck < cq) if h == 0 else (ck > cq)
                s = jnp.where(before | ((ck == cq) & (col % seg <= row % seg)), s, NEG)
            at = pl.ds(xp * rows, rows)
            m_new = jnp.broadcast_to(jnp.max(s, axis=1, keepdims=True) * scale2, (rows, 128))
            if not first:
                m_prev = m_s[qs, hh, at]
                m_new = jnp.maximum(m_prev, m_new)
                alpha = jnp.exp2(m_prev - m_new)
            m_s[qs, hh, at] = m_new
            ps = [jnp.exp2(s[:, i * 128:(i + 1) * 128] * scale2 - m_new) for i in range(keys // 128)]
            lp = ps[0]
            for v in ps[1:]:
                lp = lp + v
            p = jnp.concatenate([v.astype(jnp.bfloat16) for v in ps], axis=1)
            val = jnp.concatenate([vb[h, gg].reshape(4 * seg, 128) for gg in ggs], axis=0)
            pv = jnp.dot(p, val, preferred_element_type=jnp.float32)
            if first:
                l_s[qs, hh, at] = lp
                acc_s[qs, hh, at] = pv
            else:
                l_s[qs, hh, at] = l_s[qs, hh, at] * alpha + lp
                acc_s[qs, hh, at] = acc_s[qs, hh, at] * alpha + pv

    def ready(gg):
        arrived(kb.at[1 - c, gg], kp_rs.at[gg])
        arrived(vb.at[1 - c, gg], vp_rs.at[gg])

    def later(ggs, hh):
        todo = []
        for n in range(0, len(ggs), 2):
            pair = ggs[n:n + 2]
            todo += [(pair, 1, 0, False, False, hh, xp) for xp in range(2)]
            for gg in pair:
                h = (gg > g).astype(jnp.int32)
                todo += [([gg], h, h, False, False, hh, xp) for xp in range(2)]
        return todo

    def corner(i):
        return group(ring_step(i // 3), ring_step(i % 3))

    def pass_corner(i):
        gg = corner(i)
        arrived(kb.at[c, gg], k_rs.at[gg])
        arrived(vb.at[c, gg], v_rs.at[gg])
        to_partner(gg)

    pl.semaphore_wait(hop.at[0], 3)
    for d in STEPS:
        pl.semaphore_signal(hop.at[1], inc=1, device_id=dev(x, y, z + d, c), device_id_type=MESH)
    ready(g)
    near = [group(1, 0), group(0, 1), group(3, 0), group(0, 3)]

    def first_phase(hh, _):
        arrived(qb.at[hh], q_rs.at[hh])
        tiles([([g], qs, hf, masked, first, hh, xp) for qs, hf, masked, first in ((1, 0, False, True), (0, 0, True, True), (1, 1, True, False)) for xp in range(2)])

        @pl.when(hh == 0)
        def _():
            pass_direct(0)
            pass_direct(1)
            for gg in near:
                ready(gg)

        @pl.when(hh == 1)
        def _():
            pass_direct(2)

        tiles(later(near, hh))
        return 0

    lax.fori_loop(0, heads, first_phase, 0)

    pass_corner(0)
    pass_corner(1)

    def second_phase(i, _):
        first_c = corner(jnp.maximum(2 * i - 2, 0))
        second_c = corner(jnp.maximum(2 * i - 1, 0))
        pair = [jnp.where(i == 0, group(2, 0), first_c), jnp.where(i == 0, group(0, 2), second_c)]
        for gg in pair:
            ready(gg)
        tiles([u for hh in range(heads // 2) for u in later(pair, hh)])
        pass_corner(2 * i + 2)
        pass_corner(2 * i + 3)
        tiles([u for hh in range(heads // 2, heads) for u in later(pair, hh)])
        return 0

    lax.fori_loop(0, 3, second_phase, 0)

    pass_corner(8)
    last = [corner(i) for i in range(4, 9)]
    for gg in last:
        ready(gg)

    def o_move(hh, start):
        for i in range(4):
            move(so.at[hh, i], ob.at[hh, (x % 2) * 2 + c], o_ss.at[hh, i], o_rs.at[hh], i, x // 2, start)

    def third_phase(hh, _):
        tiles(later(last, hh))
        for qs in range(2):
            for xp in range(2):
                at = pl.ds(xp * rows, rows)
                out = (acc_s[qs, hh, at] / jnp.sum(l_s[qs, hh, at], axis=1, keepdims=True)).astype(so.dtype)
                for n in range(2):
                    so[hh, 2 * xp + n, qs * seg:(qs + 1) * seg, :] = out[n * seg:(n + 1) * seg]
        o_move(hh, True)
        return 0

    lax.fori_loop(0, heads, third_phase, 0)

    n_blk = 4
    wide = part.shape[3] // n_blk

    def cols(b):
        return pl.ds(b * wide, wide)

    def joined(b):
        return pltpu.make_async_remote_copy(src_ref=part.at[:, 1 - c, :, cols(b)], dst_ref=jb.at[:, :, cols(b)], send_sem=j_ss.at[b], recv_sem=j_rs.at[b], device_id=dev(x, y, z, 1 - c), device_id_type=MESH)

    for hh in range(heads):
        wo_loads[hh].wait()
        arrived(ob.at[hh], o_rs.at[hh])
        o_rows = jnp.concatenate([ob[hh, i] for i in range(4)], axis=1)
        for b in range(n_blk):
            term = jnp.dot(o_rows, wo[hh, :, :, b * wide:(b + 1) * wide].reshape(4 * 128, wide), preferred_element_type=jnp.float32)
            at = slice(b * wide, (b + 1) * wide)
            term = term.reshape(2, 2, half, wide)
            part[:, :, :, at] = term if hh == 0 else part[:, :, :, at] + term
            if hh == heads - 1:
                joined(b).start()
    for b in range(n_blk):
        joined(b).wait()
        at = slice(b * wide, (b + 1) * wide)
        for n in range(2):
            own_rows = slice(n * half, (n + 1) * half)
            h_ref[own_rows, at] = (x_ref[own_rows, at].astype(jnp.float32) + (part[n, c, :, at] + jb[n, :, at])).astype(h_ref.dtype)

    n_dev, cap, width = send.shape
    n_grp = s_rs.shape[0]
    per = n_dev // n_grp
    rows = per * cap
    for copy in loads:
        copy.wait()

    def pack(lo):
        at = lax.broadcasted_iota(jnp.int32, (seg, st_ref.shape[1]), 0) + lo * seg
        pick = (at == st_ref[0:1, :]) | (at == st_ref[1:2, :])
        out = jnp.dot(pick.astype(jnp.bfloat16), h_ref[...], preferred_element_type=jnp.float32)
        send[pl.ds(lo * (seg // cap), seg // cap)] = out.astype(jnp.bfloat16).reshape(seg // cap, cap, width)

    for lo in range(n_dev * cap // seg):
        pack(lo)

    pl.semaphore_wait(hop.at[1], 3)

    def peer(k, sign):
        j = (k * 91) % n_dev
        xx = (x + sign * ((j // 2) % 4)) % 4
        yy = (y + sign * ((j // 8) % 4)) % 4
        zz = (z + sign * (j // 32)) % 4
        return zz * 16 + yy * 4 + xx, (c + j) % 2

    def give(k, _):
        pc, t = peer(k, 1)
        pltpu.make_async_remote_copy(src_ref=send.at[pc * 2 + t], dst_ref=recv.at[k], send_sem=s_ss, recv_sem=s_rs.at[k // per], device_id=(0, pc, t), device_id_type=MESH).start()
        return 0

    own = pltpu.make_async_copy(send.at[me], recv.at[0], s_rs.at[0])
    own.start()
    lax.fori_loop(1, n_dev, give, 0)

    def answer(k, _):
        pc, t = peer(k, 3)
        pltpu.make_async_remote_copy(src_ref=res.at[k], dst_ref=back.at[me], send_sem=r_ss, recv_sem=r_rs, device_id=(0, pc, t), device_id_type=MESH).start()
        return 0

    def group(i, _):
        part = recv.at[pl.ds(i * per, per)]
        pltpu.make_async_copy(part, part, s_rs.at[i]).wait()
        rows_in = part[...].reshape(rows, width)
        gate = jnp.dot(rows_in, wg[...], preferred_element_type=jnp.float32)
        up = jnp.dot(rows_in, wu[...], preferred_element_type=jnp.float32)
        act = (jax.nn.silu(gate) * up).astype(jnp.bfloat16)
        out = jnp.dot(act, wd[...], preferred_element_type=jnp.float32)
        res[pl.ds(i * per, per)] = out.astype(jnp.bfloat16).reshape(per, cap, width)
        lax.fori_loop(jnp.maximum(i * per, 1), (i + 1) * per, answer, 0)
        return 0

    lax.fori_loop(0, n_grp, group, 0)
    own_back = pltpu.make_async_copy(res.at[0], back.at[me], r_rs)
    own_back.start()
    pltpu.make_async_copy(back, back, r_rs).wait()
    all_back = back[...].reshape(n_dev * cap, width)
    at = lax.broadcasted_iota(jnp.int32, (s_ref.shape[0], n_dev * cap), 1)
    total = h_ref[...].astype(jnp.float32)
    moe = None
    for j in range(2):
        pick = (at == s_ref[:, j:j + 1]).astype(jnp.bfloat16)
        term = g_ref[:, j:j + 1] * jnp.dot(pick, all_back, preferred_element_type=jnp.float32)
        moe = term if moe is None else moe + term
    y_ref[...] = (total + moe).astype(y_ref.dtype)
    most = send.at[pl.ds(1, n_dev - 1)]
    pltpu.make_async_copy(most, most, s_ss).wait()
    pltpu.make_async_copy(most, most, r_ss).wait()
    exchange(False)
    for hh in range(heads):
        o_move(hh, False)
    arrived(kb.at[0, pl.ds(0, 6)], kd_ss)
    arrived(vb.at[0, pl.ds(0, 6)], vd_ss)
    arrived(kb.at[0, pl.ds(0, 9)], kf_ss)
    arrived(vb.at[0, pl.ds(0, 9)], vf_ss)
    arrived(kb.at[0], kp_ss)
    arrived(vb.at[0], vp_ss)


def block(q, kt, val, x_blk, slot_ids, gates, w_o, w_gate, w_up, w_down, cap):
    rows, cols = q.shape
    seg = kt.shape[-1]
    heads = cols // 512
    tok_dev, d_model = x_blk.shape
    ff = w_gate.shape[1]
    n_dev = 4 * tok_dev // cap
    n_grp = 8
    dma = pltpu.SemaphoreType.DMA
    bf, f32 = jnp.bfloat16, jnp.float32
    vm = pl.BlockSpec(memory_space=pltpu.VMEM)
    hbm = pl.BlockSpec(memory_space=pltpu.HBM)
    buf = pltpu.VMEM((n_dev, cap, d_model), bf)
    return pl.pallas_call(
        functools.partial(block_kernel, (128 ** -0.5) * math.log2(math.e)),
        out_shape=jax.ShapeDtypeStruct(x_blk.shape, bf),
        in_specs=[vm] * 7 + [hbm] * 4,
        out_specs=vm,
        scratch_shapes=[
            pltpu.VMEM((heads, 4, rows, 128), bf),
            pltpu.VMEM((2, 16, 4, seg, 128), bf),
            pltpu.VMEM((2, 16, 4, seg, 128), bf),
            pltpu.VMEM((heads, 4, rows, 128), bf),
            pltpu.VMEM((heads, 4, rows, 128), bf),
            pltpu.VMEM((heads, 4, 128, d_model), bf),
            pltpu.VMEM((2, 2, tok_dev // 2, d_model), f32),
            pltpu.VMEM((2, tok_dev // 2, d_model), f32),
            pltpu.VMEM((2, heads, 4 * seg, 128), f32),
            pltpu.VMEM((2, heads, 4 * seg, 128), f32),
            pltpu.VMEM((2, heads, 4 * seg, 128), f32),
            pltpu.VMEM(x_blk.shape, bf),
            buf, buf, buf, buf,
            pltpu.VMEM((d_model, ff), bf), pltpu.VMEM((d_model, ff), bf), pltpu.VMEM((ff, d_model), bf),
            dma((3,)), pltpu.SemaphoreType.REGULAR((2,)), dma, dma((n_grp,)), dma, dma,
            dma((heads,)), dma((heads, 4)), dma((4,)), dma((4,)), dma((heads, 4)),
            dma((heads,)), dma, dma, dma((heads,)),
            dma((16,)), dma((16,)), dma((16,)), dma((16,)),
            dma, dma, dma, dma, dma, dma, dma((4,)), dma((4,)),
        ],
        compiler_params=pltpu.CompilerParams(collective_id=3, has_side_effects=True, vmem_limit_bytes=52 * 1024 * 1024),
        name='ring_block',
    )(q, kt, val, x_blk, slot_ids.T, slot_ids, gates, w_o.reshape(4, heads, 128, d_model), w_gate, w_up, w_down)


def solution(mesh):
    cp_size = mesh.shape['cp']
    tp_size = mesh.shape['tp']
    num_devs = cp_size * tp_size
    row_spec = P(('data', 'cp', 'tp'), None)
    head_spec = P(None, 'tp', None)
    wo_spec = P('tp', None, None)
    expert_spec = P(('cp', 'tp'), None, None)

    def device_fn(x_blk, w_q, w_k, w_v, w_o, idx_blk, gate_blk, w_gate, w_up, w_down):
        tok_dev, d_model = x_blk.shape
        exp_local = w_gate.shape[0]
        num_exp = exp_local * num_devs
        capacity = 4 * tok_dev // num_exp

        x_rows = swap_rows(x_blk)
        x_seg = x_rows.reshape(2, tok_dev, d_model)
        key_t = jnp.einsum('mnc,hsm->nhcs', w_k, x_seg, preferred_element_type=jnp.float32).astype(jnp.bfloat16)
        val = jnp.einsum('hsm,mnc->nhsc', x_seg, w_v, preferred_element_type=jnp.float32).astype(jnp.bfloat16)
        queries = jnp.dot(x_rows, w_q.reshape(d_model, -1), preferred_element_type=jnp.float32).astype(jnp.bfloat16)
        flat_ids = idx_blk.reshape(-1)
        onehot = (flat_ids[:, None] == jnp.arange(num_exp)[None, :]).astype(jnp.int32)
        slot_pos = jnp.sum(jnp.cumsum(onehot, axis=0) * onehot, axis=1) - 1
        slot_ids = (flat_ids * capacity + slot_pos).reshape(tok_dev, 2)
        return block(queries, key_t, val, x_blk, slot_ids, gate_blk, w_o, w_gate[0], w_up[0], w_down[0], capacity)

    return jax.shard_map(device_fn, mesh=mesh, in_specs=(row_spec, head_spec, head_spec, head_spec, wo_spec, row_spec, row_spec, expert_spec, expert_spec, expert_spec), out_specs=row_spec, check_vma=False)
```
